256 devices in a mesh: dp: 8 (over z), space: 32 (over x, y, core).
Axes of the slice: x: 4, y: 4, z: 8, core: 2. Of those that a mesh axis runs over, the one named last changes fastest.
Arguments:
- voxels: bfloat16 [131072, 256], P(('dp', 'space')), may hold values from -6 to 6
- counts: int32 [512], P(('dp', 'space')), may hold values from 32 to 256
- partners: int32 [512, 3], P(('dp', 'space')), may hold values from 0 to 511, as said below
- gain_attn: float32 [256], replicated, may hold values from 0.5 to 1.5
- w_qkv: bfloat16 [256, 768], replicated, may hold values from -5 to 5
- w_out: bfloat16 [256, 256], replicated, may hold values from -0.375 to 0.375
- gain_mlp: float32 [256], replicated, may hold values from 0.5 to 1.5
- w_up: bfloat16 [256, 1024], replicated, may hold values from -0.375 to 0.375
- w_down: bfloat16 [1024, 256], replicated, may hold values from -0.1875 to 0.1875
- cotangent: bfloat16 [131072, 256], P(('dp', 'space')), may hold values from -6 to 6
Outputs:
- output: bfloat16 [131072, 256], P(('dp', 'space'))
- grad_voxels: float32 [131072, 256], P(('dp', 'space'))
- grad_qkv: float32 [256, 768], replicated
- grad_out: float32 [256, 256], replicated
- grad_up: float32 [256, 1024], replicated
- grad_down: float32 [1024, 256], replicated
- grad_gain_attn: float32 [256], replicated
- grad_gain_mlp: float32 [256], replicated
The draws below stay inside these ranges and needn't reach their ends.
Inputs may be any that keep to these rules, and one draw needn't show every extreme that they name: `partners`: blocks are numbered so that each index of dp holds a contiguous range of 512 / 8 blocks. Row i lists blocks of the same range as block i, each within 2 blocks of i and never i itself.
All inputs are finite; a program needn't handle non-finite values.
Results may differ from the reference program's by a relative error of at most 0.024.
The reference program's roundings to bfloat16 on the way (of `normed`, `packed`, `attended`, `normed_mlp`, `hidden`, `grad_pre`, `grad_attended` and `grad_packed`) count: a program that leaves them out, or rounds other values in their place, can miss the bound.
Values may be sent and summed in bfloat16 or wider, within the bound.
No kernel may reach another device: no remote copies, remote signals or barrier semaphores. Data moves between devices by JAX's collectives and lax.ppermute only.
A program may use at most 128 MiB of HBM per device.

```python
import math
import jax
import jax.numpy as jnp
from jax import lax

D = 256
HEADS = 8
HEAD = 32
FF = 1024
BS = 256
PART = 3
SPAN = 2
NBLOCKS = 512
TOKENS = 131072
N_DP = 8


def draw_partners(key, part):
    group_size = NBLOCKS // N_DP
    slots = jnp.arange(2 * SPAN, dtype=jnp.int32)
    table = jnp.where(slots < SPAN, slots - SPAN, slots - SPAN + 1)
    scores = jax.random.randint(key, (NBLOCKS, 2 * SPAN), 0, 1 << 20, dtype=jnp.int32) * (2 * SPAN) + slots[None, :]
    order = jnp.argsort(scores, axis=1)[:, :PART]
    offsets = jnp.take(table, order)
    block_ids = jnp.arange(NBLOCKS, dtype=jnp.int32)[:, None]
    inside = block_ids % group_size + offsets
    inside_ok = (inside >= 0) & (inside < group_size)
    offsets = jnp.where(inside_ok, offsets, -offsets)
    return (block_ids + offsets).astype(jnp.int32)


def draw_w_qkv(key, part):
    base = jax.random.truncated_normal(key, -3.0, 3.0, (D, 3 * D), jnp.float32) * D ** (-0.5)
    return base.astype(jnp.bfloat16)


def set_ends(result, rng, smallest, top_value):
    index_at = [jax.random.randint(jax.random.fold_in(rng, axis), (), 0, length) for axis, length in enumerate(result.shape)]
    longest = result.shape.index(max(result.shape))
    neighbour = index_at[:longest] + [(index_at[longest] + 1) % result.shape[longest]] + index_at[longest + 1:]
    return result.at[tuple(index_at)].set(smallest).at[tuple(neighbour)].set(top_value)


def steps_of(key, shape, pieces, low, largest):
    factor_of = 1.0
    for dim, parts in pieces:
        draws = jax.random.uniform(jax.random.fold_in(jax.random.fold_in(key, 6), dim), (parts,), jnp.float32, low / len(pieces), largest / len(pieces))
        factor_of = factor_of * jnp.repeat(jnp.exp(draws), shape[dim] // parts).reshape((-1,) + (1,) * (len(shape) - 1 - dim))
    return factor_of


def gaussian(key, dims, scale, bound, pieces=(), kind=jnp.bfloat16):
    gain = steps_of(key, dims, pieces, -0.22, 0.18) if pieces else 1.0
    drawn = jax.random.normal(key, dims, jnp.float32) * scale * gain
    return jnp.minimum(jnp.maximum(drawn, -bound), bound).astype(kind)


def setup_inputs(seed: int = 0) -> dict:
    key_list = jax.random.split(jax.random.key(seed), 11)
    voxels = gaussian(key_list[0], (TOKENS, D), 1.0, 6.0, ((0, 256),))
    counts = set_ends(jax.random.randint(key_list[1], (NBLOCKS,), BS // 8, BS + 1), jax.random.fold_in(key_list[1], 1), BS // 8, BS).astype(jnp.int32)
    partners = draw_partners(jax.random.fold_in(key_list[10], 71), 0)
    gain_attn = jnp.clip(1.0 + 0.1 * jax.random.normal(key_list[3], (D,), jnp.float32), 0.5, 1.5)
    w_qkv = draw_w_qkv(jax.random.fold_in(key_list[10], 71), 0)
    w_out = gaussian(key_list[5], (D, D), D ** -0.5, 0.375)
    gain_mlp = jnp.clip(1.0 + 0.1 * jax.random.normal(key_list[6], (D,), jnp.float32), 0.5, 1.5)
    w_up = gaussian(key_list[7], (D, FF), D ** -0.5, 0.375)
    w_down = gaussian(key_list[8], (FF, D), FF ** -0.5, 0.1875)
    cotangent = gaussian(key_list[9], (TOKENS, D), 1.0, 6.0, ((0, 256),))
    return dict(voxels=voxels, counts=counts, partners=partners, gain_attn=gain_attn, w_qkv=w_qkv, w_out=w_out, gain_mlp=gain_mlp, w_up=w_up, w_down=w_down, cotangent=cotangent)


epsilon = 1e-06
root_coef = math.sqrt(2.0 / math.pi)

def matmul(left, right):
    return jnp.dot(left, right, preferred_element_type=jnp.float32)

def outer_sum(left, right):
    return jnp.einsum('rd,re->de', left.astype(jnp.float32), right.astype(jnp.float32), precision=lax.Precision.HIGHEST)

def product(form, left, right):
    return jnp.einsum(form, left.astype(jnp.float32), right.astype(jnp.float32), precision=lax.Precision.HIGHEST)

def gelu_value(pre_act):
    tangent = jnp.tanh(root_coef * (pre_act + 0.044715 * pre_act * pre_act * pre_act))
    return 0.5 * pre_act * (1.0 + tangent)

def gelu_slope(pre_act):
    tangent = jnp.tanh(root_coef * (pre_act + 0.044715 * pre_act * pre_act * pre_act))
    return 0.5 * (1.0 + tangent) + 0.5 * pre_act * (1.0 - tangent * tangent) * root_coef * (1.0 + 3.0 * 0.044715 * pre_act * pre_act)

def norm_rows(row_values, gain_vec):
    inv_rms = lax.rsqrt(lax.optimization_barrier(jnp.mean(row_values * row_values, axis=-1, keepdims=True)) + epsilon)
    return (inv_rms, (row_values * inv_rms * gain_vec).astype(jnp.bfloat16))

def norm_back(row_values, inv_rms, gain_vec, grad_norm):
    scaled_grad = grad_norm * gain_vec
    grad_rows = inv_rms * (scaled_grad - row_values * inv_rms * inv_rms * lax.optimization_barrier(jnp.mean(scaled_grad * row_values, axis=-1, keepdims=True)))
    return (grad_rows, lax.optimization_barrier(jnp.sum(grad_norm * row_values * inv_rms, axis=0)))

def attend_weights(query, key_heads, key_valid):
    scores = product('qhd,khd->hqk', query, key_heads) / math.sqrt(query.shape[-1])
    scores = jnp.where(key_valid[None, None, :], scores, -1e+30)
    row_max = lax.optimization_barrier(jnp.max(scores, axis=-1, keepdims=True))
    expo = jnp.exp(scores - row_max)
    return expo / lax.optimization_barrier(jnp.sum(expo, axis=-1, keepdims=True))

def attend_forward(query, key_heads, value_heads, key_valid):
    weights = attend_weights(query, key_heads, key_valid).astype(jnp.bfloat16)
    return product('hqk,khd->qhd', weights, value_heads).astype(jnp.bfloat16)

def attend_backward(query, key_heads, value_heads, key_valid, grad_result):
    weights = attend_weights(query, key_heads, key_valid)
    weights_b = weights.astype(jnp.bfloat16)
    grad_values = product('hqk,qhd->khd', weights_b, grad_result)
    grad_w = product('qhd,khd->hqk', grad_result, value_heads)
    grad_scores = weights * (grad_w - lax.optimization_barrier(jnp.sum(weights * grad_w, axis=-1, keepdims=True))) / math.sqrt(query.shape[-1])
    grad_scores = grad_scores.astype(jnp.bfloat16)
    grad_query = product('hqk,khd->qhd', grad_scores, key_heads)
    grad_keys = product('hqk,qhd->khd', grad_scores, query)
    return (grad_query, grad_keys, grad_values)

def reference(voxels, counts, partners, gain_attn, w_qkv, w_out, gain_mlp, w_up, w_down, cotangent):
    row_values = voxels.astype(jnp.float32)
    inv_attn, normed = norm_rows(row_values, gain_attn)
    packed = matmul(normed, w_qkv).astype(jnp.bfloat16)
    blocks = packed.reshape(NBLOCKS, BS, 3 * D)
    query_blocks = blocks[:, :, :D].reshape(NBLOCKS, BS, HEADS, HEAD)
    pair_blocks = blocks[:, :, D:]
    chosen = jnp.concatenate([jnp.arange(NBLOCKS, dtype=jnp.int32)[:, None], partners.astype(jnp.int32)], axis=1)
    position = jnp.arange(BS, dtype=jnp.int32)

    def keys_of(block_index):
        picked = jnp.take(pair_blocks, chosen[block_index], axis=0)
        key_valid = (position[None, :] < jnp.take(counts, chosen[block_index])[:, None]).reshape(-1)
        key_heads = picked[:, :, :D].reshape((PART + 1) * BS, HEADS, HEAD)
        value_heads = picked[:, :, D:].reshape((PART + 1) * BS, HEADS, HEAD)
        return (key_heads, value_heads, key_valid)

    def forward_block(block_index):
        key_heads, value_heads, key_valid = keys_of(block_index)
        return attend_forward(query_blocks[block_index], key_heads, value_heads, key_valid)
    attended = lax.map(forward_block, jnp.arange(NBLOCKS, dtype=jnp.int32)).reshape(TOKENS, D)
    mixed = row_values + matmul(attended, w_out)
    inv_mlp, normed_mlp = norm_rows(mixed, gain_mlp)
    pre_act = matmul(normed_mlp, w_up)
    hidden = gelu_value(pre_act).astype(jnp.bfloat16)
    output = (mixed + matmul(hidden, w_down)).astype(jnp.bfloat16)
    upstream = cotangent.astype(jnp.float32)
    down_sum = outer_sum(hidden, cotangent)
    grad_pre = (matmul(cotangent, w_down.T) * gelu_slope(pre_act)).astype(jnp.bfloat16)
    up_sum = outer_sum(normed_mlp, grad_pre)
    grad_normed_mlp = matmul(grad_pre, w_up.T)
    grad_through, gain_mlp_sum = norm_back(mixed, inv_mlp, gain_mlp, grad_normed_mlp)
    grad_mixed = upstream + grad_through
    grad_mixed_b = grad_mixed.astype(jnp.bfloat16)
    out_sum = outer_sum(attended, grad_mixed_b)
    grad_attended = matmul(grad_mixed_b, w_out.T).astype(jnp.bfloat16).reshape(NBLOCKS, BS, HEADS, HEAD)

    def backward_block(grad_acc, block_index):
        key_heads, value_heads, key_valid = keys_of(block_index)
        grad_query, grad_keys, grad_values = attend_backward(query_blocks[block_index], key_heads, value_heads, key_valid, grad_attended[block_index])
        stacked = jnp.concatenate([grad_keys.reshape(PART + 1, BS, D), grad_values.reshape(PART + 1, BS, D)], axis=-1)
        for member in range(PART + 1):
            grad_acc = grad_acc.at[chosen[block_index, member]].add(stacked[member])
        return (grad_acc, grad_query)
    grad_pairs, grad_queries = lax.scan(backward_block, jnp.zeros((NBLOCKS, BS, 2 * D), jnp.float32), jnp.arange(NBLOCKS, dtype=jnp.int32))
    grad_packed = jnp.concatenate([grad_queries.reshape(TOKENS, D), grad_pairs.reshape(TOKENS, 2 * D)], axis=-1).astype(jnp.bfloat16)
    qkv_sum = outer_sum(normed, grad_packed)
    grad_normed = matmul(grad_packed, w_qkv.T)
    grad_rows, gain_attn_sum = norm_back(row_values, inv_attn, gain_attn, grad_normed)
    grad_voxels = grad_mixed + grad_rows
    factor = 1.0 / math.sqrt(TOKENS)
    return (output, grad_voxels, qkv_sum * factor, out_sum * factor, up_sum * factor, down_sum * factor, gain_attn_sum * factor, gain_mlp_sum * factor)
```

```python
import math

import jax
import jax.numpy as jnp
from jax import lax
from jax.experimental import pallas as pl
from jax.experimental.pallas import tpu as pltpu
from jax.sharding import PartitionSpec as P

HEADS = 8
HEAD = 32
BS = 256
PART = 3
SPAN = 2
SLOTS = PART + 1
D = 256
FF = 1024
LANES = 128
CROWS = 8
EXTRA = 16

epsilon = 1e-06
root_coef = math.sqrt(2.0 / math.pi)
F32 = jnp.float32
BF16 = jnp.bfloat16
SCORE = 1.0 / math.sqrt(HEAD)
SCORE2 = math.log2(math.e) / math.sqrt(HEAD)


def mm(a, b):
    return lax.dot_general(a, b, (((1,), (0,)), ((), ())), preferred_element_type=F32)


def mm_t(a, b):
    return lax.dot_general(a, b, (((1,), (1,)), ((), ())), preferred_element_type=F32)


def t_mm(a, b):
    return lax.dot_general(a, b, (((0,), (0,)), ((), ())), preferred_element_type=F32)


def put_rows(ref, at, per, vals):
    for i in range(vals.shape[0] // 64):
        r = at + i * 64
        ref[r // per, r % per : r % per + 64, :] = vals[i * 64 : (i + 1) * 64, :]


def main_kernel(local_blocks, rel, xa, lo, hi, gain_attn, w_qkv, w_out, gain_mlp, w_up, w_down, cot,
                output, grads, to_lo, to_hi, gn_own, gm_out,
                cnt_s, normed_s, xhat_s, k_s, v_s, kt_s, vt_s, qbt_s, gbt_s, qb_s, gb_s,
                e_s, ds_s, ot_s, linv_s, del_s, dk_s, dv_s, dqt_s, gnm_s, mix_s, oacc_s):
    nb = local_blocks
    ext = nb + 2 * SPAN
    rows = nb * BS
    per = grads.shape[1] - EXTRA
    g_attn = gain_attn[...]
    g_mlp = gain_mlp[...]
    zero_tile = jnp.zeros((D, BS), BF16)
    lane_head = lax.broadcasted_iota(jnp.int32, (1, D), 1) // HEAD

    for blk in range(ext):
        if blk < SPAN:
            src, at = lo, blk
        elif blk < SPAN + nb:
            src, at = xa, blk - SPAN
        else:
            src, at = hi, blk - SPAN - nb
        x = src[at * BS : (at + 1) * BS, :].astype(F32)
        inv = lax.rsqrt(jnp.mean(x * x, axis=-1, keepdims=True) + epsilon)
        xhat = x * inv
        xhat_s[blk] = xhat
        normed = (xhat * g_attn).astype(BF16)
        normed_s[blk] = normed
        cnt_s[blk] = src[rows + at * CROWS : rows + (at + 1) * CROWS, :].astype(F32)
        k = mm(normed, w_qkv[:, D : 2 * D])
        k_s[blk] = k.astype(BF16)
        kt_s[blk] = k.T.astype(BF16)
        v = mm(normed, w_qkv[:, 2 * D :])
        v_s[blk] = v.astype(BF16)
        vt_s[blk] = v.T.astype(BF16)
        if SPAN <= blk < SPAN + nb:
            q = mm(normed, w_qkv[:, :D])
            qt = q.T.astype(BF16)
            for h in range(HEADS):
                qb_s[at, h] = jnp.where(lane_head == h, q, 0.0).astype(BF16)
                qbt_s[at, h] = zero_tile
                gbt_s[at, h] = zero_tile
                qbt_s[at, h, h * HEAD : (h + 1) * HEAD, :] = qt[h * HEAD : (h + 1) * HEAD, :]
        dk_s[blk] = jnp.zeros((BS, D), F32)
        dv_s[blk] = jnp.zeros((BS, D), F32)

    row_id = lax.broadcasted_iota(jnp.int32, (BS, BS), 0).astype(F32)

    def slots(b):
        return [b + SPAN] + [rel[b, j] for j in range(PART)]

    def forward(step, carry):
        b = step // HEADS
        h = step % HEADS
        ids = slots(b)
        qt = qbt_s[b, h]
        scores = []
        top = None
        for j in range(SLOTS):
            s = mm(k_s[ids[j]], qt)
            s = jnp.where(row_id < cnt_s[ids[j]][0:1, :], s, -1e30)
            scores.append(s)
            m = jnp.max(s, axis=0, keepdims=True)
            top = m if top is None else jnp.maximum(top, m)
        total = None
        out = None
        hs = pl.multiple_of(h * HEAD, HEAD)
        for j in range(SLOTS):
            e = jnp.exp2((scores[j] - top) * SCORE2)
            t = jnp.sum(e, axis=0, keepdims=True)
            total = t if total is None else total + t
            eb = e.astype(BF16)
            e_s[b, h, j] = eb
            o = mm(vt_s[ids[j], pl.ds(hs, HEAD), :], eb)
            out = o if out is None else out + o
        linv = 1.0 / total
        linv_s[step] = linv
        ot_s[b, pl.ds(hs, HEAD), :] = out * linv
        return carry

    lax.fori_loop(0, nb * HEADS, forward, 0)

    for b in range(nb):
        att = ot_s[b].astype(BF16)
        x = xa[b * BS : (b + 1) * BS, :].astype(F32)
        mixed = x + t_mm(att, w_out[...])
        mix_s[b * BS : (b + 1) * BS, :] = mixed
    mixed = mix_s[...]
    inv_m = lax.rsqrt(jnp.mean(mixed * mixed, axis=-1, keepdims=True) + epsilon)
    nm = (mixed * inv_m * g_mlp).astype(BF16)
    ct = cot[...]
    at_up = 3 * D * D // LANES
    at_down = at_up + D * FF // LANES
    at_out = at_down + D * FF // LANES
    chunk = 256
    for c in range(FF // chunk):
        cs = slice(c * chunk, (c + 1) * chunk)
        pre = mm(nm, w_up[:, cs])
        sq = pre * pre
        tangent = jnp.tanh(root_coef * (pre + 0.044715 * sq * pre))
        half = 0.5 * (1.0 + tangent)
        hidden = (pre * half).astype(BF16)
        slope = half + 0.5 * pre * (1.0 - tangent * tangent) * root_coef * (
            1.0 + 3.0 * 0.044715 * sq
        )
        o = mm(hidden, w_down[cs, :])
        gp = (mm_t(ct, w_down[cs, :]) * slope).astype(BF16)
        g = mm_t(gp, w_up[:, cs])
        if c == 0:
            oacc_s[...] = o
            gnm_s[...] = g
        else:
            oacc_s[...] += o
            gnm_s[...] += g
        down = t_mm(hidden, ct).astype(BF16)
        up = t_mm(nm, gp).astype(BF16)
        for i in range(D // LANES):
            put_rows(grads, at_down + i * FF + c * chunk, per, down[:, i * LANES : (i + 1) * LANES])
        for i in range(chunk // LANES):
            put_rows(grads, at_up + (c * (chunk // LANES) + i) * D, per, up[:, i * LANES : (i + 1) * LANES])
    output[...] = (mixed + oacc_s[...]).astype(BF16)
    gnm = gnm_s[...]
    scaled = gnm * g_mlp
    gm = ct.astype(F32) + inv_m * (
        scaled - mixed * (inv_m * inv_m) * jnp.mean(scaled * mixed, axis=-1, keepdims=True)
    )
    gm_out[...] = gm
    gain_mlp_sum = jnp.sum(gnm * mixed * inv_m, axis=0, keepdims=True)
    gmb = gm.astype(BF16)
    out_sum = None
    for b in range(nb):
        g_b = gmb[b * BS : (b + 1) * BS, :]
        o = mm(ot_s[b].astype(BF16), g_b)
        out_sum = o if out_sum is None else out_sum + o
        gt = mm_t(w_out[...], g_b).astype(BF16).astype(F32)
        pieces = []
        for h in range(HEADS):
            hs = slice(h * HEAD, (h + 1) * HEAD)
            gh = (gt[hs, :] * linv_s[b * HEADS + h]).astype(BF16)
            gbt_s[b, h, hs, :] = gh
            gf = gh.astype(F32)
            pieces.append(gf)
            del_s[b * HEADS + h] = jnp.sum(gf * ot_s[b, hs, :], axis=0, keepdims=True)
        gq = jnp.concatenate(pieces, axis=0).T
        for h in range(HEADS):
            gb_s[b, h] = jnp.where(lane_head == h, gq, 0.0).astype(BF16)
    out_sum = out_sum.astype(BF16)
    for i in range(D // LANES):
        put_rows(grads, at_out + i * D, per, out_sum[:, i * LANES : (i + 1) * LANES])

    def backward(step, carry):
        b = step // HEADS
        h = step % HEADS
        ids = slots(b)
        gt = gbt_s[b, h]
        delta = del_s[step]
        hs = pl.multiple_of(h * HEAD, HEAD)
        dq = None
        for j in range(SLOTS):
            gw = mm(v_s[ids[j]], gt)
            ds = (e_s[b, h, j].astype(F32) * (gw - delta)).astype(BF16)
            ds_s[b, h, j] = ds
            q = mm(kt_s[ids[j], pl.ds(hs, HEAD), :], ds)
            dq = q if dq is None else dq + q
        dqt_s[b, pl.ds(hs, HEAD), :] = dq * SCORE
        return carry

    lax.fori_loop(0, nb * HEADS, backward, 0)

    def key_grads(step, carry):
        b = step // SLOTS
        j = step % SLOTS
        at = jnp.where(j == 0, b + SPAN, rel[b, jnp.maximum(j - 1, 0)])
        dv = None
        dk = None
        for h in range(HEADS):
            a = mm(e_s[b, h, j], gb_s[b, h])
            dv = a if dv is None else dv + a
        for h in range(HEADS):
            a = mm(ds_s[b, h, j], qb_s[b, h])
            dk = a if dk is None else dk + a
        dv_s[at] += dv
        dk_s[at] += dk
        return carry

    lax.fori_loop(0, nb * SLOTS, key_grads, 0)

    wq = w_qkv[:, :D]
    wk = w_qkv[:, D : 2 * D]
    wv = w_qkv[:, 2 * D :]
    sums = [None, None, None]
    gain_sum = None
    for blk in range(ext):
        normed = normed_s[blk]
        dk = (dk_s[blk] * SCORE).astype(BF16)
        dv = dv_s[blk].astype(BF16)
        gn = mm_t(dk, wk) + mm_t(dv, wv)
        parts = [(1, dk), (2, dv)]
        if SPAN <= blk < SPAN + nb:
            dq = dqt_s[blk - SPAN].T.astype(BF16)
            gn = gn + mm_t(dq, wq)
            parts.append((0, dq))
            gn_own[(blk - SPAN) * BS : (blk - SPAN + 1) * BS, :] = gn
        elif blk < SPAN:
            to_lo[blk * BS : (blk + 1) * BS, :] = gn.astype(BF16)
        else:
            to_hi[(blk - SPAN - nb) * BS : (blk - SPAN - nb + 1) * BS, :] = gn.astype(BF16)
        for which, val in parts:
            a = t_mm(normed, val)
            sums[which] = a if sums[which] is None else sums[which] + a
        g = jnp.sum(gn * xhat_s[blk], axis=0, keepdims=True)
        gain_sum = g if gain_sum is None else gain_sum + g
    for which in range(3):
        s = sums[which].astype(BF16)
        for i in range(D // LANES):
            put_rows(grads, (which * (D // LANES) + i) * D, per, s[:, i * LANES : (i + 1) * LANES])
    for r in range(grads.shape[0]):
        grads[r, per:, :] = jnp.zeros((EXTRA, LANES), BF16)
    for i in range(D // LANES):
        ls = slice(i * LANES, (i + 1) * LANES)
        grads[i, per:, :] = jnp.broadcast_to(gain_sum[:, ls], (EXTRA, LANES)).astype(BF16)
        grads[D // LANES + i, per:, :] = jnp.broadcast_to(gain_mlp_sum[:, ls], (EXTRA, LANES)).astype(BF16)


def back_kernel(xa, gm, gn_own, from_lo, from_hi, gain_attn, grad_voxels):
    rows = gm.shape[0]
    x = xa[:rows, :].astype(F32)
    inv = lax.rsqrt(jnp.mean(x * x, axis=-1, keepdims=True) + epsilon)
    gn = gn_own[...] + from_lo[...].astype(F32) + from_hi[...].astype(F32)
    scaled = gn * gain_attn[...]
    grad_voxels[...] = gm[...] + inv * (
        scaled - x * (inv * inv) * jnp.mean(scaled * x, axis=-1, keepdims=True)
    )


def get_rows(ref, at, per, count):
    out = []
    for i in range(count // 64):
        r = at + i * 64
        out.append(ref[r // per, r % per : r % per + 64, :].astype(F32))
    return jnp.concatenate(out, axis=0)


def unpack_kernel(factor, summed, grad_qkv, grad_out, grad_up, grad_down, grad_ga, grad_gm):
    per = summed.shape[1] - EXTRA
    at_up = 3 * D * D // LANES
    at_down = at_up + D * FF // LANES
    at_out = at_down + D * FF // LANES
    for i in range(3 * D // LANES):
        grad_qkv[:, i * LANES : (i + 1) * LANES] = get_rows(summed, i * D, per, D) * factor
    for i in range(FF // LANES):
        grad_up[:, i * LANES : (i + 1) * LANES] = get_rows(summed, at_up + i * D, per, D) * factor
    for i in range(D // LANES):
        ls = slice(i * LANES, (i + 1) * LANES)
        grad_down[:, ls] = get_rows(summed, at_down + i * FF, per, FF) * factor
        grad_out[:, ls] = get_rows(summed, at_out + i * D, per, D) * factor
        grad_ga[:, ls] = summed[i, per : per + 1, :].astype(F32) * factor
        grad_gm[:, ls] = summed[D // LANES + i, per : per + 1, :].astype(F32) * factor


def sum_kernel(arrived, spread):
    total = arrived[0].astype(F32)
    for i in range(1, arrived.shape[0]):
        total = total + arrived[i].astype(F32)
    total = total.astype(BF16)
    for i in range(spread.shape[0]):
        spread[i] = total


VM = pl.BlockSpec(memory_space=pltpu.VMEM)
SM = pl.BlockSpec(memory_space=pltpu.SMEM)
PARAMS = pltpu.CompilerParams(vmem_limit_bytes=60 * 1024 * 1024)


def sds(shape, dtype):
    return jax.ShapeDtypeStruct(shape, dtype)


def sum_spread(arrived, copies):
    return pl.pallas_call(
        sum_kernel,
        out_shape=sds((copies, *arrived.shape[1:]), BF16),
        in_specs=[VM],
        out_specs=VM,
        compiler_params=PARAMS,
        name="sum_spread",
    )(arrived)


def exchange(x, axis):
    return lax.all_to_all(x, axis, split_axis=0, concat_axis=0, tiled=True)


def body(voxels, counts, partners, gain_attn, w_qkv, w_out, gain_mlp, w_up, w_down, cotangent):
    nb = counts.shape[0]
    rows = voxels.shape[0]
    n_space = lax.axis_size("space")
    n_dp = lax.axis_size("dp")
    first_block = (lax.axis_index("dp") * n_space + lax.axis_index("space")) * nb
    up = [(i, i + 1) for i in range(n_space - 1)]
    down = [(j, i) for i, j in up]
    marks = jnp.broadcast_to(counts.astype(BF16)[:, None, None], (nb, CROWS, D)).reshape(nb * CROWS, D)
    xa = jnp.concatenate([voxels, marks], axis=0)
    lo = lax.ppermute(xa, "space", up)
    hi = lax.ppermute(xa, "space", down)
    rel = partners - (first_block - SPAN)
    ext = nb + 2 * SPAN
    per = (3 * D * D + D * D + 2 * D * FF) // LANES // n_space
    tile = (BS, D)
    scratch = [
        pltpu.VMEM((ext, CROWS, D), F32),
        pltpu.VMEM((ext, *tile), BF16),
        pltpu.VMEM((ext, *tile), F32),
        pltpu.VMEM((ext, *tile), BF16),
        pltpu.VMEM((ext, *tile), BF16),
        pltpu.VMEM((ext, *tile), BF16),
        pltpu.VMEM((ext, *tile), BF16),
        pltpu.VMEM((nb, HEADS, *tile), BF16),
        pltpu.VMEM((nb, HEADS, *tile), BF16),
        pltpu.VMEM((nb, HEADS, *tile), BF16),
        pltpu.VMEM((nb, HEADS, *tile), BF16),
        pltpu.VMEM((nb, HEADS, SLOTS, BS, BS), BF16),
        pltpu.VMEM((nb, HEADS, SLOTS, BS, BS), BF16),
        pltpu.VMEM((nb, *tile), F32),
        pltpu.VMEM((nb * HEADS, 1, BS), F32),
        pltpu.VMEM((nb * HEADS, 1, BS), F32),
        pltpu.VMEM((ext, *tile), F32),
        pltpu.VMEM((ext, *tile), F32),
        pltpu.VMEM((nb, *tile), F32),
        pltpu.VMEM((rows, D), F32),
        pltpu.VMEM((rows, D), F32),
        pltpu.VMEM((rows, D), F32),
    ]
    ga = gain_attn.reshape(1, D)
    gmlp = gain_mlp.reshape(1, D)
    output, grads, to_lo, to_hi, gn_own, gm = pl.pallas_call(
        lambda *refs: main_kernel(nb, *refs),
        out_shape=[
            sds((rows, D), BF16),
            sds((n_space, per + EXTRA, LANES), BF16),
            sds((rows, D), BF16),
            sds((rows, D), BF16),
            sds((rows, D), F32),
            sds((rows, D), F32),
        ],
        in_specs=[SM] + [VM] * 10,
        out_specs=[VM] * 6,
        scratch_shapes=scratch,
        compiler_params=PARAMS,
        name="layer",
    )(rel, xa, lo, hi, ga, w_qkv, w_out, gmlp, w_up, w_down, cotangent)
    from_lo = lax.ppermute(to_hi, "space", up)
    from_hi = lax.ppermute(to_lo, "space", down)
    shares = exchange(grads, "space")
    grad_voxels = pl.pallas_call(
        back_kernel,
        out_shape=sds((rows, D), F32),
        in_specs=[VM] * 6,
        out_specs=VM,
        compiler_params=PARAMS,
        name="voxel_grad",
    )(xa, gm, gn_own, from_lo, from_hi, ga)
    over_dp = exchange(sum_spread(shares, n_dp), "dp")
    summed = exchange(sum_spread(over_dp, n_space), "space")
    factor = 1.0 / math.sqrt(rows * n_dp * n_space)
    outs = pl.pallas_call(
        lambda *refs: unpack_kernel(factor, *refs),
        out_shape=[
            sds((D, 3 * D), F32),
            sds((D, D), F32),
            sds((D, FF), F32),
            sds((FF, D), F32),
            sds((1, D), F32),
            sds((1, D), F32),
        ],
        in_specs=[VM],
        out_specs=[VM] * 6,
        compiler_params=PARAMS,
        name="unpack",
    )(summed)
    grad_qkv, grad_out, grad_up, grad_down, grad_ga, grad_gm = outs
    return (output, grad_voxels, grad_qkv, grad_out, grad_up, grad_down, grad_ga.reshape(D), grad_gm.reshape(D))


def solution(mesh):
    in_specs = (
        P(("dp", "space"), None),
        P(("dp", "space")),
        P(("dp", "space"), None),
        P(),
        P(),
        P(),
        P(),
        P(),
        P(),
        P(("dp", "space"), None),
    )
    out_specs = (P(("dp", "space"), None), P(("dp", "space"), None), P(), P(), P(), P(), P(), P())
    return jax.shard_map(body, mesh=mesh, in_specs=in_specs, out_specs=out_specs, check_vma=False)
```

```python
import math

import jax
import jax.numpy as jnp
from jax import lax
from jax.experimental import pallas as pl
from jax.experimental.pallas import tpu as pltpu
from jax.sharding import Mesh, PartitionSpec as P

HEADS = 8
HEAD = 32
BS = 256
PART = 3
SPAN = 2
SLOTS = PART + 1
D = 256
FF = 1024
LANES = 128
EXTRA = 8
PIECE = 32
FAR = 128.0
SHARE = ("core", "pair", "chip")
SPACE = ("chip", "core")

epsilon = 1e-06
root_coef = math.sqrt(2.0 / math.pi)
F32 = jnp.float32
BF16 = jnp.bfloat16
SCORE = 1.0 / math.sqrt(HEAD)
SCORE2 = math.log2(math.e) / math.sqrt(HEAD)


def mm(a, b):
    return lax.dot_general(a, b, (((1,), (0,)), ((), ())), preferred_element_type=F32)


def mm_t(a, b):
    return lax.dot_general(a, b, (((1,), (1,)), ((), ())), preferred_element_type=F32)


def t_mm(a, b):
    return lax.dot_general(a, b, (((0,), (0,)), ((), ())), preferred_element_type=F32)


def put_rows(ref, at, per, vals):
    for i in range(vals.shape[0] // PIECE):
        r = at + i * PIECE
        ref[r // per, r % per : r % per + PIECE, :] = vals[i * PIECE : (i + 1) * PIECE, :]


def main_kernel(local_blocks, partners, counts, xa, lo, hi, gain_attn, w_qkv, w_out, gain_mlp, w_up, w_down, cot,
                output, grads, to_lo, to_hi, gn_own, gm_out,
                bias_s, normed_s, xhat_s, k_s, v_s, kt_s, vt_s, qbt_s, gbt_s, qb_s, gb_s,
                e_s, ds_s, ot_s, linv_s, del_s, dk_s, dv_s, dqt_s, gnm_s, mix_s, oacc_s):
    nb = local_blocks
    ext = nb + 2 * SPAN
    rows = nb * BS
    per = grads.shape[1] - EXTRA
    g_attn = gain_attn[...]
    g_mlp = gain_mlp[...]
    zero_tile = jnp.zeros((D, BS), BF16)
    place = lax.axis_index("far") * lax.axis_size("pair") + lax.axis_index("pair")
    for axis in SPACE:
        place = place * lax.axis_size(axis) + lax.axis_index(axis)
    base = place * nb - SPAN
    lane_head = lax.broadcasted_iota(jnp.int32, (1, D), 1) // HEAD
    row_id = lax.broadcasted_iota(jnp.int32, (BS, BS), 0)

    for blk in range(ext):
        if blk < SPAN:
            src, at = lo, blk
        elif blk < SPAN + nb:
            src, at = xa, blk - SPAN
        else:
            src, at = hi, blk - SPAN - nb
        x = src[at * BS : (at + 1) * BS, :].astype(F32)
        inv = lax.rsqrt(jnp.mean(x * x, axis=-1, keepdims=True) + epsilon)
        xhat = x * inv
        xhat_s[blk] = xhat
        normed = (xhat * g_attn).astype(BF16)
        normed_s[blk] = normed
        if SPAN <= blk < SPAN + nb:
            bias_s[blk] = jnp.where(row_id < counts[at], 0.0, -1e30)
        else:
            bias_s[blk] = jnp.where(x > FAR / 2, -1e30, 0.0)
        k = mm(normed, w_qkv[:, D : 2 * D])
        k_s[blk] = k.astype(BF16)
        kt_s[blk] = k.T.astype(BF16)
        v = mm(normed, w_qkv[:, 2 * D :])
        v_s[blk] = v.astype(BF16)
        vt_s[blk] = v.T.astype(BF16)
        if SPAN <= blk < SPAN + nb:
            q = mm(normed, w_qkv[:, :D])
            qt = q.T.astype(BF16)
            for h in range(HEADS):
                qb_s[at, h] = jnp.where(lane_head == h, q, 0.0).astype(BF16)
                qbt_s[at, h] = zero_tile
                gbt_s[at, h] = zero_tile
                qbt_s[at, h, h * HEAD : (h + 1) * HEAD, :] = qt[h * HEAD : (h + 1) * HEAD, :]
        dk_s[blk] = jnp.zeros((BS, D), F32)
        dv_s[blk] = jnp.zeros((BS, D), F32)

    def slots(b):
        return [b + SPAN] + [partners[b, j] - base for j in range(PART)]

    def forward(step, carry):
        b = step // HEADS
        h = step % HEADS
        ids = slots(b)
        qt = qbt_s[b, h]
        scores = []
        top = None
        for j in range(SLOTS):
            s = mm(k_s[ids[j]], qt)
            s = s + bias_s[ids[j]]
            scores.append(s)
            m = jnp.max(s, axis=0, keepdims=True)
            top = m if top is None else jnp.maximum(top, m)
        total = None
        out = None
        hs = pl.multiple_of(h * HEAD, HEAD)
        for j in range(SLOTS):
            e = jnp.exp2((scores[j] - top) * SCORE2)
            t = jnp.sum(e, axis=0, keepdims=True)
            total = t if total is None else total + t
            eb = e.astype(BF16)
            e_s[b, h, j] = eb
            o = mm(vt_s[ids[j], pl.ds(hs, HEAD), :], eb)
            out = o if out is None else out + o
        linv = 1.0 / total
        linv_s[step] = linv
        ot_s[b, pl.ds(hs, HEAD), :] = out * linv
        return carry

    lax.fori_loop(0, nb * HEADS, forward, 0)

    for b in range(nb):
        att = ot_s[b].astype(BF16)
        x = xa[b * BS : (b + 1) * BS, :].astype(F32)
        mixed = x + t_mm(att, w_out[...])
        mix_s[b * BS : (b + 1) * BS, :] = mixed
    mixed = mix_s[...]
    inv_m = lax.rsqrt(jnp.mean(mixed * mixed, axis=-1, keepdims=True) + epsilon)
    nm = (mixed * inv_m * g_mlp).astype(BF16)
    ct = cot[...]
    at_up = 3 * D * D // LANES
    at_down = at_up + D * FF // LANES
    at_out = at_down + D * FF // LANES
    chunk = 256
    for c in range(FF // chunk):
        cs = slice(c * chunk, (c + 1) * chunk)
        pre = mm(nm, w_up[:, cs])
        sq = pre * pre
        tangent = jnp.tanh(root_coef * (pre + 0.044715 * sq * pre))
        half = 0.5 * (1.0 + tangent)
        hidden = (pre * half).astype(BF16)
        slope = half + 0.5 * pre * (1.0 - tangent * tangent) * root_coef * (
            1.0 + 3.0 * 0.044715 * sq
        )
        o = mm(hidden, w_down[cs, :])
        gp = (mm_t(ct, w_down[cs, :]) * slope).astype(BF16)
        g = mm_t(gp, w_up[:, cs])
        if c == 0:
            oacc_s[...] = o
            gnm_s[...] = g
        else:
            oacc_s[...] += o
            gnm_s[...] += g
        down = t_mm(hidden, ct).astype(BF16)
        up = t_mm(nm, gp).astype(BF16)
        for i in range(D // LANES):
            put_rows(grads, at_down + i * FF + c * chunk, per, down[:, i * LANES : (i + 1) * LANES])
        for i in range(chunk // LANES):
            put_rows(grads, at_up + (c * (chunk // LANES) + i) * D, per, up[:, i * LANES : (i + 1) * LANES])
    output[...] = (mixed + oacc_s[...]).astype(BF16)
    gnm = gnm_s[...]
    scaled = gnm * g_mlp
    gm = ct.astype(F32) + inv_m * (
        scaled - mixed * (inv_m * inv_m) * jnp.mean(scaled * mixed, axis=-1, keepdims=True)
    )
    gm_out[...] = gm
    gain_mlp_sum = jnp.sum(gnm * mixed * inv_m, axis=0, keepdims=True)
    gmb = gm.astype(BF16)
    out_sum = None
    for b in range(nb):
        g_b = gmb[b * BS : (b + 1) * BS, :]
        o = mm(ot_s[b].astype(BF16), g_b)
        out_sum = o if out_sum is None else out_sum + o
        gt = mm_t(w_out[...], g_b).astype(BF16).astype(F32)
        pieces = []
        for h in range(HEADS):
            hs = slice(h * HEAD, (h + 1) * HEAD)
            gh = (gt[hs, :] * linv_s[b * HEADS + h]).astype(BF16)
            gbt_s[b, h, hs, :] = gh
            gf = gh.astype(F32)
            pieces.append(gf)
            del_s[b * HEADS + h] = jnp.sum(gf * ot_s[b, hs, :], axis=0, keepdims=True)
        gq = jnp.concatenate(pieces, axis=0).T
        for h in range(HEADS):
            gb_s[b, h] = jnp.where(lane_head == h, gq, 0.0).astype(BF16)
    out_sum = out_sum.astype(BF16)
    for i in range(D // LANES):
        put_rows(grads, at_out + i * D, per, out_sum[:, i * LANES : (i + 1) * LANES])

    def backward(step, carry):
        b = step // HEADS
        h = step % HEADS
        ids = slots(b)
        gt = gbt_s[b, h]
        delta = del_s[step]
        hs = pl.multiple_of(h * HEAD, HEAD)
        dq = None
        for j in range(SLOTS):
            gw = mm(v_s[ids[j]], gt)
            ds = (e_s[b, h, j].astype(F32) * (gw - delta)).astype(BF16)
            ds_s[b, h, j] = ds
            q = mm(kt_s[ids[j], pl.ds(hs, HEAD), :], ds)
            dq = q if dq is None else dq + q
        dqt_s[b, pl.ds(hs, HEAD), :] = dq * SCORE
        return carry

    lax.fori_loop(0, nb * HEADS, backward, 0)

    def key_grads(step, carry):
        b = step // SLOTS
        j = step % SLOTS
        at = jnp.where(j == 0, b + SPAN, partners[b, jnp.maximum(j - 1, 0)] - base)
        dv = None
        dk = None
        for h in range(HEADS):
            a = mm(e_s[b, h, j], gb_s[b, h])
            dv = a if dv is None else dv + a
        for h in range(HEADS):
            a = mm(ds_s[b, h, j], qb_s[b, h])
            dk = a if dk is None else dk + a
        dv_s[at] += dv
        dk_s[at] += dk
        return carry

    lax.fori_loop(0, nb * SLOTS, key_grads, 0)

    wq = w_qkv[:, :D]
    wk = w_qkv[:, D : 2 * D]
    wv = w_qkv[:, 2 * D :]
    sums = [None, None, None]
    gain_sum = None
    for blk in range(ext):
        normed = normed_s[blk]
        dk = (dk_s[blk] * SCORE).astype(BF16)
        dv = dv_s[blk].astype(BF16)
        gn = mm_t(dk, wk) + mm_t(dv, wv)
        parts = [(1, dk), (2, dv)]
        if SPAN <= blk < SPAN + nb:
            dq = dqt_s[blk - SPAN].T.astype(BF16)
            gn = gn + mm_t(dq, wq)
            parts.append((0, dq))
            gn_own[(blk - SPAN) * BS : (blk - SPAN + 1) * BS, :] = gn
        elif blk < SPAN:
            to_lo[blk * BS : (blk + 1) * BS, :] = gn.astype(BF16)
        else:
            to_hi[(blk - SPAN - nb) * BS : (blk - SPAN - nb + 1) * BS, :] = gn.astype(BF16)
        for which, val in parts:
            a = t_mm(normed, val)
            sums[which] = a if sums[which] is None else sums[which] + a
        g = jnp.sum(gn * xhat_s[blk], axis=0, keepdims=True)
        gain_sum = g if gain_sum is None else gain_sum + g
    for which in range(3):
        s = sums[which].astype(BF16)
        for i in range(D // LANES):
            put_rows(grads, (which * (D // LANES) + i) * D, per, s[:, i * LANES : (i + 1) * LANES])
    for r in range(grads.shape[0]):
        grads[r, per:, :] = jnp.zeros((EXTRA, LANES), BF16)
    for i in range(D // LANES):
        ls = slice(i * LANES, (i + 1) * LANES)
        grads[i, per:, :] = jnp.broadcast_to(gain_sum[:, ls], (EXTRA, LANES)).astype(BF16)
        grads[D // LANES + i, per:, :] = jnp.broadcast_to(gain_mlp_sum[:, ls], (EXTRA, LANES)).astype(BF16)


def back_kernel(xa, gm, gn_own, from_lo, from_hi, gain_attn, grad_voxels):
    rows = gm.shape[0]
    x = xa[:rows, :].astype(F32)
    inv = lax.rsqrt(jnp.mean(x * x, axis=-1, keepdims=True) + epsilon)
    gn = gn_own[...] + from_lo[...].astype(F32) + from_hi[...].astype(F32)
    scaled = gn * gain_attn[...]
    grad_voxels[...] = gm[...] + inv * (
        scaled - x * (inv * inv) * jnp.mean(scaled * x, axis=-1, keepdims=True)
    )


def get_rows(halves, at, per, count):
    half = halves[0].shape[0]
    out = []
    for i in range(count // PIECE):
        r = at + i * PIECE
        share = r // per
        ref = halves[share // half]
        out.append(ref[share % half, r % per : r % per + PIECE, :].astype(F32))
    return jnp.concatenate(out, axis=0)


def unpack_kernel(factor, mine, theirs, grad_qkv, grad_out, grad_up, grad_down, grad_ga, grad_gm):
    per = mine.shape[1] - EXTRA
    at_up = 3 * D * D // LANES
    at_down = at_up + D * FF // LANES
    at_out = at_down + D * FF // LANES

    def unpack(halves):
        for i in range(3 * D // LANES):
            grad_qkv[:, i * LANES : (i + 1) * LANES] = get_rows(halves, i * D, per, D) * factor
        for i in range(FF // LANES):
            grad_up[:, i * LANES : (i + 1) * LANES] = get_rows(halves, at_up + i * D, per, D) * factor
        for i in range(D // LANES):
            ls = slice(i * LANES, (i + 1) * LANES)
            grad_down[:, ls] = get_rows(halves, at_down + i * FF, per, FF) * factor
            grad_out[:, ls] = get_rows(halves, at_out + i * D, per, D) * factor
            grad_ga[:, ls] = halves[0][i, per : per + 1, :].astype(F32) * factor
            grad_gm[:, ls] = halves[0][D // LANES + i, per : per + 1, :].astype(F32) * factor

    core = lax.axis_index("core")
    pl.when(core == 0)(lambda: unpack((mine, theirs)))
    pl.when(core != 0)(lambda: unpack((theirs, mine)))


def sum_kernel(arrived, spread):
    total = arrived[0].astype(F32)
    for i in range(1, arrived.shape[0]):
        total = total + arrived[i].astype(F32)
    total = total.astype(BF16)
    for i in range(spread.shape[0]):
        spread[i] = total


VM = pl.BlockSpec(memory_space=pltpu.VMEM)
SM = pl.BlockSpec(memory_space=pltpu.SMEM)
PARAMS = pltpu.CompilerParams(vmem_limit_bytes=60 * 1024 * 1024)


def sds(shape, dtype):
    return jax.ShapeDtypeStruct(shape, dtype)


def sum_spread(arrived, copies):
    return pl.pallas_call(
        sum_kernel,
        out_shape=sds((copies, *arrived.shape[1:]), BF16),
        in_specs=[VM],
        out_specs=VM,
        compiler_params=PARAMS,
        name="sum_spread",
    )(arrived)


def exchange(x, axis):
    return lax.all_to_all(x, axis, split_axis=0, concat_axis=0, tiled=True)


def body(voxels, counts, partners, gain_attn, w_qkv, w_out, gain_mlp, w_up, w_down, cotangent):
    nb = counts.shape[0]
    rows = voxels.shape[0]
    n_space = lax.axis_size(SPACE)
    n_share = lax.axis_size(SHARE)
    n_far = lax.axis_size("far")
    up = [(i, i + 1) for i in range(n_space - 1)]
    down = [(j, i) for i, j in up]
    held = lax.broadcasted_iota(jnp.int32, (nb, BS, D), 1) < counts[:, None, None]
    marked = jnp.where(held, voxels.reshape(nb, BS, D), jnp.asarray(FAR, BF16)).reshape(rows, D)
    lo = lax.ppermute(marked, SPACE, up)
    hi = lax.ppermute(marked, SPACE, down)
    ext = nb + 2 * SPAN
    per = (3 * D * D + D * D + 2 * D * FF) // LANES // n_share
    tile = (BS, D)
    scratch = [
        pltpu.VMEM((ext, *tile), F32),
        pltpu.VMEM((ext, *tile), BF16),
        pltpu.VMEM((ext, *tile), F32),
        pltpu.VMEM((ext, *tile), BF16),
        pltpu.VMEM((ext, *tile), BF16),
        pltpu.VMEM((ext, *tile), BF16),
        pltpu.VMEM((ext, *tile), BF16),
        pltpu.VMEM((nb, HEADS, *tile), BF16),
        pltpu.VMEM((nb, HEADS, *tile), BF16),
        pltpu.VMEM((nb, HEADS, *tile), BF16),
        pltpu.VMEM((nb, HEADS, *tile), BF16),
        pltpu.VMEM((nb, HEADS, SLOTS, BS, BS), BF16),
        pltpu.VMEM((nb, HEADS, SLOTS, BS, BS), BF16),
        pltpu.VMEM((nb, *tile), F32),
        pltpu.VMEM((nb * HEADS, 1, BS), F32),
        pltpu.VMEM((nb * HEADS, 1, BS), F32),
        pltpu.VMEM((ext, *tile), F32),
        pltpu.VMEM((ext, *tile), F32),
        pltpu.VMEM((nb, *tile), F32),
        pltpu.VMEM((rows, D), F32),
        pltpu.VMEM((rows, D), F32),
        pltpu.VMEM((rows, D), F32),
    ]
    ga = gain_attn.reshape(1, D)
    gmlp = gain_mlp.reshape(1, D)
    output, grads, to_lo, to_hi, gn_own, gm = pl.pallas_call(
        lambda *refs: main_kernel(nb, *refs),
        out_shape=[
            sds((rows, D), BF16),
            sds((n_share, per + EXTRA, LANES), BF16),
            sds((rows, D), BF16),
            sds((rows, D), BF16),
            sds((rows, D), F32),
            sds((rows, D), F32),
        ],
        in_specs=[SM, SM] + [VM] * 10,
        out_specs=[VM] * 6,
        scratch_shapes=scratch,
        compiler_params=PARAMS,
        name="layer",
    )(partners, counts, voxels, lo, hi, ga, w_qkv, w_out, gmlp, w_up, w_down, cotangent)
    shares = exchange(grads, SHARE)
    to_lo, to_hi, shares = lax.optimization_barrier((to_lo, to_hi, shares))
    from_lo = lax.ppermute(to_hi, SPACE, up)
    from_hi = lax.ppermute(to_lo, SPACE, down)
    over_far = exchange(sum_spread(shares, n_far), "far")
    spread = sum_spread(over_far, n_share // 2)
    spread, from_lo, from_hi = lax.optimization_barrier((spread, from_lo, from_hi))
    mine = exchange(spread, ("pair", "chip"))
    grad_voxels = pl.pallas_call(
        back_kernel,
        out_shape=sds((rows, D), F32),
        in_specs=[VM] * 6,
        out_specs=VM,
        compiler_params=PARAMS,
        cost_estimate=pl.CostEstimate(flops=4000000, transcendentals=0, bytes_accessed=3000000),
        name="voxel_grad",
    )(voxels, gm, gn_own, from_lo, from_hi, ga)
    theirs = lax.ppermute(mine, "core", [(0, 1), (1, 0)])
    factor = 1.0 / math.sqrt(rows * n_far * lax.axis_size("pair") * n_space)
    outs = pl.pallas_call(
        lambda *refs: unpack_kernel(factor, *refs),
        out_shape=[
            sds((D, 3 * D), F32),
            sds((D, D), F32),
            sds((D, FF), F32),
            sds((FF, D), F32),
            sds((1, D), F32),
            sds((1, D), F32),
        ],
        in_specs=[VM] * 2,
        out_specs=[VM] * 6,
        compiler_params=PARAMS,
        name="unpack",
    )(mine, theirs)
    grad_qkv, grad_out, grad_up, grad_down, grad_ga, grad_gm = outs
    return (output, grad_voxels, grad_qkv, grad_out, grad_up, grad_down, grad_ga.reshape(D), grad_gm.reshape(D))


def solution(mesh):
    n_dp, n_space = mesh.devices.shape
    fine = Mesh(mesh.devices.reshape(n_dp // 2, 2, n_space // 2, 2), ("far", "pair", "chip", "core"))
    row = ("far", "pair", "chip", "core")
    in_specs = (
        P(row, None),
        P(row),
        P(row, None),
        P(),
        P(),
        P(),
        P(),
        P(),
        P(),
        P(row, None),
    )
    out_specs = (P(row, None), P(row, None), P(), P(), P(), P(), P(), P())
    return jax.shard_map(body, mesh=fine, in_specs=in_specs, out_specs=out_specs, check_vma=False)
```

```python
import math

import jax
import jax.numpy as jnp
from jax import lax
from jax.experimental import pallas as pl
from jax.experimental.pallas import tpu as pltpu
from jax.sharding import Mesh, PartitionSpec as P

HEADS = 8
HEAD = 32
BS = 256
PART = 3
SPAN = 2
SLOTS = PART + 1
D = 256
FF = 1024
LANES = 128
EXTRA = 8
PIECE = 32
FAR = 128.0
SHARE = ("core", "pair", "chip")
SPACE = ("chip", "core")

epsilon = 1e-06
root_coef = math.sqrt(2.0 / math.pi)
F32 = jnp.float32
BF16 = jnp.bfloat16
SCORE = 1.0 / math.sqrt(HEAD)
SCORE2 = math.log2(math.e) / math.sqrt(HEAD)


def mm(a, b):
    return lax.dot_general(a, b, (((1,), (0,)), ((), ())), preferred_element_type=F32)


def mm_t(a, b):
    return lax.dot_general(a, b, (((1,), (1,)), ((), ())), preferred_element_type=F32)


def t_mm(a, b):
    return lax.dot_general(a, b, (((0,), (0,)), ((), ())), preferred_element_type=F32)


def put_rows(ref, at, per, vals):
    for i in range(vals.shape[0] // PIECE):
        r = at + i * PIECE
        ref[r // per, r % per : r % per + PIECE, :] = vals[i * PIECE : (i + 1) * PIECE, :]


def main_kernel(local_blocks, partners, counts, xa, lo, hi, gain_attn, w_qkv, w_out, gain_mlp, w_up, w_down, cot,
                output, grads, to_lo, to_hi, gn_own, gm_out,
                bias_s, normed_s, xhat_s, k_s, v_s, kt_s, vt_s, qbt_s, gbt_s, qb_s, gb_s,
                s_s, e_s, ds_s, ot_s, linv_s, del_s, dk_s, dv_s, dqt_s, gnm_s, mix_s, oacc_s):
    nb = local_blocks
    ext = nb + 2 * SPAN
    per = grads.shape[1] - EXTRA
    g_attn = gain_attn[...]
    g_mlp = gain_mlp[...]
    zero_tile = jnp.zeros((D, BS), BF16)
    place = lax.axis_index("far") * lax.axis_size("pair") + lax.axis_index("pair")
    for axis in SPACE:
        place = place * lax.axis_size(axis) + lax.axis_index(axis)
    base = place * nb - SPAN
    lane_head = lax.broadcasted_iota(jnp.int32, (1, D), 1) // HEAD
    row_id = lax.broadcasted_iota(jnp.int32, (BS, BS), 0)

    for blk in range(ext):
        if blk < SPAN:
            src, at = lo, blk
        elif blk < SPAN + nb:
            src, at = xa, blk - SPAN
        else:
            src, at = hi, blk - SPAN - nb
        x = src[at * BS : (at + 1) * BS, :].astype(F32)
        inv = lax.rsqrt(jnp.mean(x * x, axis=-1, keepdims=True) + epsilon)
        xhat = x * inv
        xhat_s[blk] = xhat
        normed = (xhat * g_attn).astype(BF16)
        normed_s[blk] = normed
        if SPAN <= blk < SPAN + nb:
            bias_s[blk] = jnp.where(row_id < counts[at], 0.0, -1e30)
        else:
            bias_s[blk] = jnp.where(x > FAR / 2, -1e30, 0.0)
        k = mm(normed, w_qkv[:, D : 2 * D])
        k_s[blk] = k.astype(BF16)
        kt_s[blk] = k.T.astype(BF16)
        v = mm(normed, w_qkv[:, 2 * D :])
        v_s[blk] = v.astype(BF16)
        vt_s[blk] = v.T.astype(BF16)
        if SPAN <= blk < SPAN + nb:
            q = mm(normed, w_qkv[:, :D])
            qt = q.T.astype(BF16)
            for h in range(HEADS):
                qb_s[at, h] = jnp.where(lane_head == h, q, 0.0).astype(BF16)
                qbt_s[at, h] = zero_tile
                gbt_s[at, h] = zero_tile
                qbt_s[at, h, h * HEAD : (h + 1) * HEAD, :] = qt[h * HEAD : (h + 1) * HEAD, :]
        dk_s[blk] = jnp.zeros((BS, D), F32)
        dv_s[blk] = jnp.zeros((BS, D), F32)

    def slots(b):
        return [b + SPAN] + [partners[b, j] - base for j in range(PART)]

    steps = [(b, h) for b in range(nb) for h in range(HEADS)]
    ids = [slots(b) for b in range(nb)]

    def group(x):
        return x.reshape(BS // 8, 8, BS)

    def score(t):
        b, h = steps[t]
        top = None
        for j in range(SLOTS):
            s = mm(k_s[ids[b][j]], qbt_s[b, h]) + bias_s[ids[b][j]]
            s_s[t % 2, j] = s
            m = jnp.max(group(s), axis=0)
            top = m if top is None else jnp.maximum(top, m)
        return jnp.max(top, axis=0, keepdims=True)

    def weigh(t, top):
        b, h = steps[t]
        total = None
        for j in range(SLOTS):
            e = jnp.exp2((s_s[t % 2, j] - top) * SCORE2)
            e_s[b, h, j] = e.astype(BF16)
            p = jnp.sum(group(e), axis=0)
            total = p if total is None else total + p
        return 1.0 / jnp.sum(total, axis=0, keepdims=True)

    def gather(t, linv):
        b, h = steps[t]
        hs = slice(h * HEAD, (h + 1) * HEAD)
        out = None
        for j in range(SLOTS):
            o = mm(vt_s[ids[b][j], hs, :], e_s[b, h, j])
            out = o if out is None else out + o
        linv_s[t] = linv
        ot_s[b, hs, :] = out * linv

    tops, linvs = {}, {}
    for t in range(len(steps) + 2):
        if t < len(steps):
            tops[t] = score(t)
        if 1 <= t <= len(steps):
            linvs[t - 1] = weigh(t - 1, tops.pop(t - 1))
        if t >= 2:
            gather(t - 2, linvs.pop(t - 2))

    for b in range(nb):
        att = ot_s[b].astype(BF16)
        x = xa[b * BS : (b + 1) * BS, :].astype(F32)
        mixed = x + t_mm(att, w_out[...])
        mix_s[b * BS : (b + 1) * BS, :] = mixed
    mixed = mix_s[...]
    inv_m = lax.rsqrt(jnp.mean(mixed * mixed, axis=-1, keepdims=True) + epsilon)
    nm = (mixed * inv_m * g_mlp).astype(BF16)
    ct = cot[...]
    at_up = 3 * D * D // LANES
    at_down = at_up + D * FF // LANES
    at_out = at_down + D * FF // LANES
    chunk = 256
    for c in range(FF // chunk):
        cs = slice(c * chunk, (c + 1) * chunk)
        pre = mm(nm, w_up[:, cs])
        sq = pre * pre
        tangent = jnp.tanh(root_coef * (pre + 0.044715 * sq * pre))
        half = 0.5 * (1.0 + tangent)
        hidden = (pre * half).astype(BF16)
        slope = half + 0.5 * pre * (1.0 - tangent * tangent) * root_coef * (
            1.0 + 3.0 * 0.044715 * sq
        )
        o = mm(hidden, w_down[cs, :])
        gp = (mm_t(ct, w_down[cs, :]) * slope).astype(BF16)
        g = mm_t(gp, w_up[:, cs])
        if c == 0:
            oacc_s[...] = o
            gnm_s[...] = g
        else:
            oacc_s[...] += o
            gnm_s[...] += g
        down = t_mm(hidden, ct).astype(BF16)
        up = t_mm(nm, gp).astype(BF16)
        for i in range(D // LANES):
            put_rows(grads, at_down + i * FF + c * chunk, per, down[:, i * LANES : (i + 1) * LANES])
        for i in range(chunk // LANES):
            put_rows(grads, at_up + (c * (chunk // LANES) + i) * D, per, up[:, i * LANES : (i + 1) * LANES])
    output[...] = (mixed + oacc_s[...]).astype(BF16)
    gnm = gnm_s[...]
    scaled = gnm * g_mlp
    gm = ct.astype(F32) + inv_m * (
        scaled - mixed * (inv_m * inv_m) * jnp.mean(scaled * mixed, axis=-1, keepdims=True)
    )
    gm_out[...] = gm
    gain_mlp_sum = jnp.sum(gnm * mixed * inv_m, axis=0, keepdims=True)
    gmb = gm.astype(BF16)
    out_sum = None
    for b in range(nb):
        g_b = gmb[b * BS : (b + 1) * BS, :]
        o = mm(ot_s[b].astype(BF16), g_b)
        out_sum = o if out_sum is None else out_sum + o
        gt = mm_t(w_out[...], g_b).astype(BF16).astype(F32)
        pieces = []
        for h in range(HEADS):
            hs = slice(h * HEAD, (h + 1) * HEAD)
            gh = (gt[hs, :] * linv_s[b * HEADS + h]).astype(BF16)
            gbt_s[b, h, hs, :] = gh
            gf = gh.astype(F32)
            pieces.append(gf)
            del_s[b * HEADS + h] = jnp.sum(gf * ot_s[b, hs, :], axis=0, keepdims=True)
        gq = jnp.concatenate(pieces, axis=0).T
        for h in range(HEADS):
            gb_s[b, h] = jnp.where(lane_head == h, gq, 0.0).astype(BF16)
    out_sum = out_sum.astype(BF16)
    for i in range(D // LANES):
        put_rows(grads, at_out + i * D, per, out_sum[:, i * LANES : (i + 1) * LANES])

    def score_grad(t):
        b, h = steps[t]
        for j in range(SLOTS):
            gw = mm(v_s[ids[b][j]], gbt_s[b, h])
            ds_s[b, h, j] = (e_s[b, h, j].astype(F32) * (gw - del_s[t])).astype(BF16)

    def query_grad(t):
        b, h = steps[t]
        hs = slice(h * HEAD, (h + 1) * HEAD)
        dq = None
        for j in range(SLOTS):
            q = mm(kt_s[ids[b][j], hs, :], ds_s[b, h, j])
            dq = q if dq is None else dq + q
        dqt_s[b, hs, :] = dq * SCORE

    for t in range(len(steps) + 1):
        if t < len(steps):
            score_grad(t)
        if t >= 1:
            query_grad(t - 1)

    for b in range(nb):
        for j in range(SLOTS):
            dv = None
            dk = None
            for h in range(HEADS):
                a = mm(e_s[b, h, j], gb_s[b, h])
                dv = a if dv is None else dv + a
            for h in range(HEADS):
                a = mm(ds_s[b, h, j], qb_s[b, h])
                dk = a if dk is None else dk + a
            dv_s[ids[b][j]] += dv
            dk_s[ids[b][j]] += dk

    wq = w_qkv[:, :D]
    wk = w_qkv[:, D : 2 * D]
    wv = w_qkv[:, 2 * D :]
    sums = [None, None, None]
    gain_sum = None
    for blk in range(ext):
        normed = normed_s[blk]
        dk = (dk_s[blk] * SCORE).astype(BF16)
        dv = dv_s[blk].astype(BF16)
        gn = mm_t(dk, wk) + mm_t(dv, wv)
        parts = [(1, dk), (2, dv)]
        if SPAN <= blk < SPAN + nb:
            dq = dqt_s[blk - SPAN].T.astype(BF16)
            gn = gn + mm_t(dq, wq)
            parts.append((0, dq))
            gn_own[(blk - SPAN) * BS : (blk - SPAN + 1) * BS, :] = gn
        elif blk < SPAN:
            to_lo[blk * BS : (blk + 1) * BS, :] = gn.astype(BF16)
        else:
            to_hi[(blk - SPAN - nb) * BS : (blk - SPAN - nb + 1) * BS, :] = gn.astype(BF16)
        for which, val in parts:
            a = t_mm(normed, val)
            sums[which] = a if sums[which] is None else sums[which] + a
        g = jnp.sum(gn * xhat_s[blk], axis=0, keepdims=True)
        gain_sum = g if gain_sum is None else gain_sum + g
    for which in range(3):
        s = sums[which].astype(BF16)
        for i in range(D // LANES):
            put_rows(grads, (which * (D // LANES) + i) * D, per, s[:, i * LANES : (i + 1) * LANES])
    for r in range(grads.shape[0]):
        grads[r, per:, :] = jnp.zeros((EXTRA, LANES), BF16)
    for i in range(D // LANES):
        ls = slice(i * LANES, (i + 1) * LANES)
        grads[i, per:, :] = jnp.broadcast_to(gain_sum[:, ls], (EXTRA, LANES)).astype(BF16)
        grads[D // LANES + i, per:, :] = jnp.broadcast_to(gain_mlp_sum[:, ls], (EXTRA, LANES)).astype(BF16)


def back_kernel(xa, gm, gn_own, from_lo, from_hi, gain_attn, grad_voxels):
    rows = gm.shape[0]
    x = xa[:rows, :].astype(F32)
    inv = lax.rsqrt(jnp.mean(x * x, axis=-1, keepdims=True) + epsilon)
    gn = gn_own[...] + from_lo[...].astype(F32) + from_hi[...].astype(F32)
    scaled = gn * gain_attn[...]
    grad_voxels[...] = gm[...] + inv * (
        scaled - x * (inv * inv) * jnp.mean(scaled * x, axis=-1, keepdims=True)
    )


def get_rows(halves, at, per, count):
    half = halves[0].shape[0]
    out = []
    for i in range(count // PIECE):
        r = at + i * PIECE
        share = r // per
        ref = halves[share // half]
        out.append(ref[share % half, r % per : r % per + PIECE, :].astype(F32))
    return jnp.concatenate(out, axis=0)


def unpack_kernel(factor, mine, theirs, grad_qkv, grad_out, grad_up, grad_down, grad_ga, grad_gm):
    per = mine.shape[1] - EXTRA
    at_up = 3 * D * D // LANES
    at_down = at_up + D * FF // LANES
    at_out = at_down + D * FF // LANES

    def unpack(halves):
        for i in range(3 * D // LANES):
            grad_qkv[:, i * LANES : (i + 1) * LANES] = get_rows(halves, i * D, per, D) * factor
        for i in range(FF // LANES):
            grad_up[:, i * LANES : (i + 1) * LANES] = get_rows(halves, at_up + i * D, per, D) * factor
        for i in range(D // LANES):
            ls = slice(i * LANES, (i + 1) * LANES)
            grad_down[:, ls] = get_rows(halves, at_down + i * FF, per, FF) * factor
            grad_out[:, ls] = get_rows(halves, at_out + i * D, per, D) * factor
            grad_ga[:, ls] = halves[0][i, per : per + 1, :].astype(F32) * factor
            grad_gm[:, ls] = halves[0][D // LANES + i, per : per + 1, :].astype(F32) * factor

    core = lax.axis_index("core")
    pl.when(core == 0)(lambda: unpack((mine, theirs)))
    pl.when(core != 0)(lambda: unpack((theirs, mine)))


def sum_kernel(arrived, spread):
    total = arrived[0].astype(F32)
    for i in range(1, arrived.shape[0]):
        total = total + arrived[i].astype(F32)
    total = total.astype(BF16)
    for i in range(spread.shape[0]):
        spread[i] = total


VM = pl.BlockSpec(memory_space=pltpu.VMEM)
SM = pl.BlockSpec(memory_space=pltpu.SMEM)
PARAMS = pltpu.CompilerParams(vmem_limit_bytes=60 * 1024 * 1024)


def sds(shape, dtype):
    return jax.ShapeDtypeStruct(shape, dtype)


def sum_spread(arrived, copies):
    return pl.pallas_call(
        sum_kernel,
        out_shape=sds((copies, *arrived.shape[1:]), BF16),
        in_specs=[VM],
        out_specs=VM,
        compiler_params=PARAMS,
        name="sum_spread",
    )(arrived)


def exchange(x, axis):
    return lax.all_to_all(x, axis, split_axis=0, concat_axis=0, tiled=True)


def body(voxels, counts, partners, gain_attn, w_qkv, w_out, gain_mlp, w_up, w_down, cotangent):
    nb = counts.shape[0]
    rows = voxels.shape[0]
    n_space = lax.axis_size(SPACE)
    n_share = lax.axis_size(SHARE)
    n_far = lax.axis_size("far")
    up = [(i, i + 1) for i in range(n_space - 1)]
    down = [(j, i) for i, j in up]
    held = lax.broadcasted_iota(jnp.int32, (nb, BS, D), 1) < counts[:, None, None]
    marked = jnp.where(held, voxels.reshape(nb, BS, D), jnp.asarray(FAR, BF16)).reshape(rows, D)
    lo = lax.ppermute(marked, SPACE, up)
    hi = lax.ppermute(marked, SPACE, down)
    ext = nb + 2 * SPAN
    per = (3 * D * D + D * D + 2 * D * FF) // LANES // n_share
    tile = (BS, D)
    scratch = [
        pltpu.VMEM((ext, *tile), F32),
        pltpu.VMEM((ext, *tile), BF16),
        pltpu.VMEM((ext, *tile), F32),
        pltpu.VMEM((ext, *tile), BF16),
        pltpu.VMEM((ext, *tile), BF16),
        pltpu.VMEM((ext, *tile), BF16),
        pltpu.VMEM((ext, *tile), BF16),
        pltpu.VMEM((nb, HEADS, *tile), BF16),
        pltpu.VMEM((nb, HEADS, *tile), BF16),
        pltpu.VMEM((nb, HEADS, *tile), BF16),
        pltpu.VMEM((nb, HEADS, *tile), BF16),
        pltpu.VMEM((2, SLOTS, BS, BS), F32),
        pltpu.VMEM((nb, HEADS, SLOTS, BS, BS), BF16),
        pltpu.VMEM((nb, HEADS, SLOTS, BS, BS), BF16),
        pltpu.VMEM((nb, *tile), F32),
        pltpu.VMEM((nb * HEADS, 1, BS), F32),
        pltpu.VMEM((nb * HEADS, 1, BS), F32),
        pltpu.VMEM((ext, *tile), F32),
        pltpu.VMEM((ext, *tile), F32),
        pltpu.VMEM((nb, *tile), F32),
        pltpu.VMEM((rows, D), F32),
        pltpu.VMEM((rows, D), F32),
        pltpu.VMEM((rows, D), F32),
    ]
    ga = gain_attn.reshape(1, D)
    gmlp = gain_mlp.reshape(1, D)
    output, grads, to_lo, to_hi, gn_own, gm = pl.pallas_call(
        lambda *refs: main_kernel(nb, *refs),
        out_shape=[
            sds((rows, D), BF16),
            sds((n_share, per + EXTRA, LANES), BF16),
            sds((rows, D), BF16),
            sds((rows, D), BF16),
            sds((rows, D), F32),
            sds((rows, D), F32),
        ],
        in_specs=[SM, SM] + [VM] * 10,
        out_specs=[VM] * 6,
        scratch_shapes=scratch,
        compiler_params=PARAMS,
        name="layer",
    )(partners, counts, voxels, lo, hi, ga, w_qkv, w_out, gmlp, w_up, w_down, cotangent)
    shares = exchange(grads, SHARE)
    spread = sum_spread(shares, n_far)
    to_lo, to_hi, spread = lax.optimization_barrier((to_lo, to_hi, spread))
    over_far = exchange(spread, "far")
    from_lo = lax.ppermute(to_hi, SPACE, up)
    from_hi = lax.ppermute(to_lo, SPACE, down)
    spread = sum_spread(over_far, n_share // 2)
    spread, from_lo, from_hi = lax.optimization_barrier((spread, from_lo, from_hi))
    mine = exchange(spread, ("pair", "chip"))
    grad_voxels = pl.pallas_call(
        back_kernel,
        out_shape=sds((rows, D), F32),
        in_specs=[VM] * 6,
        out_specs=VM,
        compiler_params=PARAMS,
        cost_estimate=pl.CostEstimate(flops=4000000, transcendentals=0, bytes_accessed=3000000),
        name="voxel_grad",
    )(voxels, gm, gn_own, from_lo, from_hi, ga)
    mine, grad_voxels = lax.optimization_barrier((mine, grad_voxels))
    theirs = lax.ppermute(mine, "core", [(0, 1), (1, 0)])
    factor = 1.0 / math.sqrt(rows * n_far * lax.axis_size("pair") * n_space)
    outs = pl.pallas_call(
        lambda *refs: unpack_kernel(factor, *refs),
        out_shape=[
            sds((D, 3 * D), F32),
            sds((D, D), F32),
            sds((D, FF), F32),
            sds((FF, D), F32),
            sds((1, D), F32),
            sds((1, D), F32),
        ],
        in_specs=[VM] * 2,
        out_specs=[VM] * 6,
        compiler_params=PARAMS,
        name="unpack",
    )(mine, theirs)
    grad_qkv, grad_out, grad_up, grad_down, grad_ga, grad_gm = outs
    return (output, grad_voxels, grad_qkv, grad_out, grad_up, grad_down, grad_ga.reshape(D), grad_gm.reshape(D))


def solution(mesh):
    n_dp, n_space = mesh.devices.shape
    fine = Mesh(mesh.devices.reshape(n_dp // 2, 2, n_space // 2, 2), ("far", "pair", "chip", "core"))
    row = ("far", "pair", "chip", "core")
    in_specs = (
        P(row, None),
        P(row),
        P(row, None),
        P(),
        P(),
        P(),
        P(),
        P(),
        P(),
        P(row, None),
    )
    out_specs = (P(row, None), P(row, None), P(), P(), P(), P(), P(), P())
    return jax.shard_map(body, mesh=fine, in_specs=in_specs, out_specs=out_specs, check_vma=False)
```

```python
import math

import jax
import jax.numpy as jnp
from jax import lax
from jax.experimental import pallas as pl
from jax.experimental.pallas import tpu as pltpu
from jax.sharding import Mesh, PartitionSpec as P

HEADS = 8
HEAD = 32
BS = 256
PART = 3
SPAN = 2
SLOTS = PART + 1
D = 256
FF = 1024
LANES = 128
EXTRA = 8
PIECE = 32
FAR = 128.0
SHARE = ("core", "pair", "chip")
SPACE = ("chip", "core")

epsilon = 1e-06
root_coef = math.sqrt(2.0 / math.pi)
F32 = jnp.float32
BF16 = jnp.bfloat16
SCORE = 1.0 / math.sqrt(HEAD)
SCORE2 = math.log2(math.e) / math.sqrt(HEAD)


def mm(a, b):
    return lax.dot_general(a, b, (((1,), (0,)), ((), ())), preferred_element_type=F32)


def mm_t(a, b):
    return lax.dot_general(a, b, (((1,), (1,)), ((), ())), preferred_element_type=F32)


def t_mm(a, b):
    return lax.dot_general(a, b, (((0,), (0,)), ((), ())), preferred_element_type=F32)


def put_rows(ref, at, per, vals):
    for i in range(vals.shape[0] // PIECE):
        r = at + i * PIECE
        ref[r // per, r % per : r % per + PIECE, :] = vals[i * PIECE : (i + 1) * PIECE, :]


def main_kernel(local_blocks, partners, counts, xa, lo, hi, gain_attn, w_qkv, w_out, gain_mlp, w_up, w_down, cot,
                output, grads, to_lo, to_hi, gn_own, gm_out,
                bias_s, normed_s, xhat_s, k_s, v_s, kt_s, vt_s, qbt_s, gbt_s, qb_s, gb_s,
                s_s, e_s, ds_s, ot_s, linv_s, del_s, dk_s, dv_s, dqt_s, gnm_s, mix_s, oacc_s):
    nb = local_blocks
    ext = nb + 2 * SPAN
    per = grads.shape[1] - EXTRA
    g_attn = gain_attn[...]
    g_mlp = gain_mlp[...]
    zero_tile = jnp.zeros((D, BS), BF16)
    place = lax.axis_index("far") * lax.axis_size("pair") + lax.axis_index("pair")
    for axis in SPACE:
        place = place * lax.axis_size(axis) + lax.axis_index(axis)
    base = place * nb - SPAN
    lane_head = lax.broadcasted_iota(jnp.int32, (1, D), 1) // HEAD
    row_id = lax.broadcasted_iota(jnp.int32, (BS, BS), 0)

    for blk in range(ext):
        if blk < SPAN:
            src, at = lo, blk
        elif blk < SPAN + nb:
            src, at = xa, blk - SPAN
        else:
            src, at = hi, blk - SPAN - nb
        x = src[at * BS : (at + 1) * BS, :].astype(F32)
        inv = lax.rsqrt(jnp.mean(x * x, axis=-1, keepdims=True) + epsilon)
        xhat = x * inv
        xhat_s[blk] = xhat
        normed = (xhat * g_attn).astype(BF16)
        normed_s[blk] = normed
        if SPAN <= blk < SPAN + nb:
            bias_s[blk] = jnp.where(row_id < counts[at], 0.0, -1e30)
        else:
            bias_s[blk] = jnp.where(x > FAR / 2, -1e30, 0.0)
        k = mm(normed, w_qkv[:, D : 2 * D])
        k_s[blk] = k.astype(BF16)
        kt_s[blk] = k.T.astype(BF16)
        v = mm(normed, w_qkv[:, 2 * D :])
        v_s[blk] = v.astype(BF16)
        vt_s[blk] = v.T.astype(BF16)
        if SPAN <= blk < SPAN + nb:
            q = mm(normed, w_qkv[:, :D])
            qt = q.T.astype(BF16)
            for h in range(HEADS):
                qb_s[at, h] = jnp.where(lane_head == h, q, 0.0).astype(BF16)
                qbt_s[at, h] = zero_tile
                gbt_s[at, h] = zero_tile
                qbt_s[at, h, h * HEAD : (h + 1) * HEAD, :] = qt[h * HEAD : (h + 1) * HEAD, :]
        dk_s[blk] = jnp.zeros((BS, D), F32)
        dv_s[blk] = jnp.zeros((BS, D), F32)

    def slots(b):
        return [b + SPAN] + [partners[b, j] - base for j in range(PART)]

    steps = [(b, h) for b in range(nb) for h in range(HEADS)]
    ids = [slots(b) for b in range(nb)]

    def group(x):
        return x.reshape(BS // 8, 8, BS)

    def score(t):
        b, h = steps[t]
        top = None
        for j in range(SLOTS):
            s = mm(k_s[ids[b][j]], qbt_s[b, h]) + bias_s[ids[b][j]]
            s_s[t % 2, j] = s
            m = jnp.max(group(s), axis=0)
            top = m if top is None else jnp.maximum(top, m)
        return jnp.max(top, axis=0, keepdims=True)

    def weigh(t, top):
        b, h = steps[t]
        total = None
        for j in range(SLOTS):
            e = jnp.exp2((s_s[t % 2, j] - top) * SCORE2)
            e_s[b, h, j] = e.astype(BF16)
            p = jnp.sum(group(e), axis=0)
            total = p if total is None else total + p
        return 1.0 / jnp.sum(total, axis=0, keepdims=True)

    def gather(t, linv):
        b, h = steps[t]
        hs = slice(h * HEAD, (h + 1) * HEAD)
        out = None
        for j in range(SLOTS):
            o = mm(vt_s[ids[b][j], hs, :], e_s[b, h, j])
            out = o if out is None else out + o
        linv_s[t] = linv
        ot_s[b, hs, :] = out * linv

    tops, linvs = {}, {}
    for t in range(len(steps) + 2):
        if t < len(steps):
            tops[t] = score(t)
        if 1 <= t <= len(steps):
            linvs[t - 1] = weigh(t - 1, tops.pop(t - 1))
        if t >= 2:
            gather(t - 2, linvs.pop(t - 2))

    for b in range(nb):
        att = ot_s[b].astype(BF16)
        x = xa[b * BS : (b + 1) * BS, :].astype(F32)
        mixed = x + t_mm(att, w_out[...])
        mix_s[b * BS : (b + 1) * BS, :] = mixed
    mixed = mix_s[...]
    inv_m = lax.rsqrt(jnp.mean(mixed * mixed, axis=-1, keepdims=True) + epsilon)
    nm = (mixed * inv_m * g_mlp).astype(BF16)
    ct = cot[...]
    at_up = 3 * D * D // LANES
    at_down = at_up + D * FF // LANES
    at_out = at_down + D * FF // LANES
    chunk = 256
    for c in range(FF // chunk):
        cs = slice(c * chunk, (c + 1) * chunk)
        pre = mm(nm, w_up[:, cs])
        sq = pre * pre
        tangent = jnp.tanh(root_coef * (pre + 0.044715 * sq * pre))
        half = 0.5 * (1.0 + tangent)
        hidden = (pre * half).astype(BF16)
        slope = half + 0.5 * pre * (1.0 - tangent * tangent) * root_coef * (
            1.0 + 3.0 * 0.044715 * sq
        )
        o = mm(hidden, w_down[cs, :])
        gp = (mm_t(ct, w_down[cs, :]) * slope).astype(BF16)
        g = mm_t(gp, w_up[:, cs])
        if c == 0:
            oacc_s[...] = o
            gnm_s[...] = g
        else:
            oacc_s[...] += o
            gnm_s[...] += g
        down = t_mm(hidden, ct).astype(BF16)
        up = t_mm(nm, gp).astype(BF16)
        for i in range(D // LANES):
            put_rows(grads, at_down + i * FF + c * chunk, per, down[:, i * LANES : (i + 1) * LANES])
        for i in range(chunk // LANES):
            put_rows(grads, at_up + (c * (chunk // LANES) + i) * D, per, up[:, i * LANES : (i + 1) * LANES])
    output[...] = (mixed + oacc_s[...]).astype(BF16)
    gnm = gnm_s[...]
    scaled = gnm * g_mlp
    gm = ct.astype(F32) + inv_m * (
        scaled - mixed * (inv_m * inv_m) * jnp.mean(scaled * mixed, axis=-1, keepdims=True)
    )
    gm_out[...] = gm
    gain_mlp_sum = jnp.sum(gnm * mixed * inv_m, axis=0, keepdims=True)
    gmb = gm.astype(BF16)
    out_sum = None
    for b in range(nb):
        g_b = gmb[b * BS : (b + 1) * BS, :]
        o = mm(ot_s[b].astype(BF16), g_b)
        out_sum = o if out_sum is None else out_sum + o
        gt = mm_t(w_out[...], g_b).astype(BF16).astype(F32)
        pieces = []
        for h in range(HEADS):
            hs = slice(h * HEAD, (h + 1) * HEAD)
            gh = (gt[hs, :] * linv_s[b * HEADS + h]).astype(BF16)
            gbt_s[b, h, hs, :] = gh
            gf = gh.astype(F32)
            pieces.append(gf)
            del_s[b * HEADS + h] = jnp.sum(gf * ot_s[b, hs, :], axis=0, keepdims=True)
        gq = jnp.concatenate(pieces, axis=0).T
        for h in range(HEADS):
            gb_s[b, h] = jnp.where(lane_head == h, gq, 0.0).astype(BF16)
    out_sum = out_sum.astype(BF16)
    for i in range(D // LANES):
        put_rows(grads, at_out + i * D, per, out_sum[:, i * LANES : (i + 1) * LANES])

    def score_grad(t):
        b, h = steps[t]
        for j in range(SLOTS):
            gw = mm(v_s[ids[b][j]], gbt_s[b, h])
            ds_s[b, h, j] = (e_s[b, h, j].astype(F32) * (gw - del_s[t])).astype(BF16)

    def query_grad(t):
        b, h = steps[t]
        hs = slice(h * HEAD, (h + 1) * HEAD)
        dq = None
        for j in range(SLOTS):
            q = mm(kt_s[ids[b][j], hs, :], ds_s[b, h, j])
            dq = q if dq is None else dq + q
        dqt_s[b, hs, :] = dq * SCORE

    for t in range(len(steps) + 1):
        if t < len(steps):
            score_grad(t)
        if t >= 1:
            query_grad(t - 1)

    for b in range(nb):
        for j in range(SLOTS):
            dv = None
            dk = None
            for h in range(HEADS):
                a = mm(e_s[b, h, j], gb_s[b, h])
                dv = a if dv is None else dv + a
            for h in range(HEADS):
                a = mm(ds_s[b, h, j], qb_s[b, h])
                dk = a if dk is None else dk + a
            dv_s[ids[b][j]] += dv
            dk_s[ids[b][j]] += dk

    wq = w_qkv[:, :D]
    wk = w_qkv[:, D : 2 * D]
    wv = w_qkv[:, 2 * D :]
    sums = [None, None, None]
    gain_sum = None
    for blk in range(ext):
        normed = normed_s[blk]
        dk = (dk_s[blk] * SCORE).astype(BF16)
        dv = dv_s[blk].astype(BF16)
        gn = mm_t(dk, wk) + mm_t(dv, wv)
        parts = [(1, dk), (2, dv)]
        if SPAN <= blk < SPAN + nb:
            dq = dqt_s[blk - SPAN].T.astype(BF16)
            gn = gn + mm_t(dq, wq)
            parts.append((0, dq))
            gn_own[(blk - SPAN) * BS : (blk - SPAN + 1) * BS, :] = gn
        elif blk < SPAN:
            to_lo[blk * BS : (blk + 1) * BS, :] = gn.astype(BF16)
        else:
            to_hi[(blk - SPAN - nb) * BS : (blk - SPAN - nb + 1) * BS, :] = gn.astype(BF16)
        for which, val in parts:
            a = t_mm(normed, val)
            sums[which] = a if sums[which] is None else sums[which] + a
        g = jnp.sum(gn * xhat_s[blk], axis=0, keepdims=True)
        gain_sum = g if gain_sum is None else gain_sum + g
    for which in range(3):
        s = sums[which].astype(BF16)
        for i in range(D // LANES):
            put_rows(grads, (which * (D // LANES) + i) * D, per, s[:, i * LANES : (i + 1) * LANES])
    for r in range(grads.shape[0]):
        grads[r, per:, :] = jnp.zeros((EXTRA, LANES), BF16)
    for i in range(D // LANES):
        ls = slice(i * LANES, (i + 1) * LANES)
        grads[i, per:, :] = jnp.broadcast_to(gain_sum[:, ls], (EXTRA, LANES)).astype(BF16)
        grads[D // LANES + i, per:, :] = jnp.broadcast_to(gain_mlp_sum[:, ls], (EXTRA, LANES)).astype(BF16)


def back_kernel(xa, gm, gn_own, from_lo, from_hi, gain_attn, grad_voxels):
    rows = gm.shape[0]
    x = xa[:rows, :].astype(F32)
    inv = lax.rsqrt(jnp.mean(x * x, axis=-1, keepdims=True) + epsilon)
    gn = gn_own[...] + from_lo[...].astype(F32) + from_hi[...].astype(F32)
    scaled = gn * gain_attn[...]
    grad_voxels[...] = gm[...] + inv * (
        scaled - x * (inv * inv) * jnp.mean(scaled * x, axis=-1, keepdims=True)
    )


def get_rows(halves, at, per, count):
    half = halves[0].shape[0]
    out = []
    for i in range(count // PIECE):
        r = at + i * PIECE
        share = r // per
        ref = halves[share // half]
        out.append(ref[share % half, r % per : r % per + PIECE, :].astype(F32))
    return jnp.concatenate(out, axis=0)


def unpack_kernel(factor, mine, theirs, grad_qkv, grad_out, grad_up, grad_down, grad_ga, grad_gm):
    per = mine.shape[1] - EXTRA
    at_up = 3 * D * D // LANES
    at_down = at_up + D * FF // LANES
    at_out = at_down + D * FF // LANES

    def unpack(halves):
        for i in range(3 * D // LANES):
            grad_qkv[:, i * LANES : (i + 1) * LANES] = get_rows(halves, i * D, per, D) * factor
        for i in range(FF // LANES):
            grad_up[:, i * LANES : (i + 1) * LANES] = get_rows(halves, at_up + i * D, per, D) * factor
        for i in range(D // LANES):
            ls = slice(i * LANES, (i + 1) * LANES)
            grad_down[:, ls] = get_rows(halves, at_down + i * FF, per, FF) * factor
            grad_out[:, ls] = get_rows(halves, at_out + i * D, per, D) * factor
            grad_ga[:, ls] = halves[0][i, per : per + 1, :].astype(F32) * factor
            grad_gm[:, ls] = halves[0][D // LANES + i, per : per + 1, :].astype(F32) * factor

    core = lax.axis_index("core")
    pl.when(core == 0)(lambda: unpack((mine, theirs)))
    pl.when(core != 0)(lambda: unpack((theirs, mine)))


VM = pl.BlockSpec(memory_space=pltpu.VMEM)
SM = pl.BlockSpec(memory_space=pltpu.SMEM)
PARAMS = pltpu.CompilerParams(vmem_limit_bytes=60 * 1024 * 1024)


def sds(shape, dtype):
    return jax.ShapeDtypeStruct(shape, dtype)


def exchange(x, axis):
    return lax.all_to_all(x, axis, split_axis=0, concat_axis=0, tiled=True)


def body(voxels, counts, partners, gain_attn, w_qkv, w_out, gain_mlp, w_up, w_down, cotangent):
    nb = counts.shape[0]
    rows = voxels.shape[0]
    n_space = lax.axis_size(SPACE)
    n_share = lax.axis_size(SHARE)
    n_far = lax.axis_size("far")
    up = [(i, i + 1) for i in range(n_space - 1)]
    down = [(j, i) for i, j in up]
    held = lax.broadcasted_iota(jnp.int32, (nb, BS, D), 1) < counts[:, None, None]
    marked = jnp.where(held, voxels.reshape(nb, BS, D), jnp.asarray(FAR, BF16)).reshape(rows, D)
    lo = lax.ppermute(marked, SPACE, up)
    hi = lax.ppermute(marked, SPACE, down)
    ext = nb + 2 * SPAN
    per = (3 * D * D + D * D + 2 * D * FF) // LANES // n_share
    tile = (BS, D)
    scratch = [
        pltpu.VMEM((ext, *tile), F32),
        pltpu.VMEM((ext, *tile), BF16),
        pltpu.VMEM((ext, *tile), F32),
        pltpu.VMEM((ext, *tile), BF16),
        pltpu.VMEM((ext, *tile), BF16),
        pltpu.VMEM((ext, *tile), BF16),
        pltpu.VMEM((ext, *tile), BF16),
        pltpu.VMEM((nb, HEADS, *tile), BF16),
        pltpu.VMEM((nb, HEADS, *tile), BF16),
        pltpu.VMEM((nb, HEADS, *tile), BF16),
        pltpu.VMEM((nb, HEADS, *tile), BF16),
        pltpu.VMEM((2, SLOTS, BS, BS), F32),
        pltpu.VMEM((nb, HEADS, SLOTS, BS, BS), BF16),
        pltpu.VMEM((nb, HEADS, SLOTS, BS, BS), BF16),
        pltpu.VMEM((nb, *tile), F32),
        pltpu.VMEM((nb * HEADS, 1, BS), F32),
        pltpu.VMEM((nb * HEADS, 1, BS), F32),
        pltpu.VMEM((ext, *tile), F32),
        pltpu.VMEM((ext, *tile), F32),
        pltpu.VMEM((nb, *tile), F32),
        pltpu.VMEM((rows, D), F32),
        pltpu.VMEM((rows, D), F32),
        pltpu.VMEM((rows, D), F32),
    ]
    ga = gain_attn.reshape(1, D)
    gmlp = gain_mlp.reshape(1, D)
    output, grads, to_lo, to_hi, gn_own, gm = pl.pallas_call(
        lambda *refs: main_kernel(nb, *refs),
        out_shape=[
            sds((rows, D), BF16),
            sds((n_share, per + EXTRA, LANES), BF16),
            sds((rows, D), BF16),
            sds((rows, D), BF16),
            sds((rows, D), F32),
            sds((rows, D), F32),
        ],
        in_specs=[SM, SM] + [VM] * 10,
        out_specs=[VM] * 6,
        scratch_shapes=scratch,
        compiler_params=PARAMS,
        name="layer",
    )(partners, counts, voxels, lo, hi, ga, w_qkv, w_out, gmlp, w_up, w_down, cotangent)
    shares = exchange(grads, SHARE)
    from_lo = lax.ppermute(to_hi, SPACE, up)
    from_hi = lax.ppermute(to_lo, SPACE, down)
    grad_voxels = pl.pallas_call(
        back_kernel,
        out_shape=sds((rows, D), F32),
        in_specs=[VM] * 6,
        out_specs=VM,
        compiler_params=PARAMS,
        cost_estimate=pl.CostEstimate(flops=4000000, transcendentals=0, bytes_accessed=3000000),
        name="voxel_grad",
    )(voxels, gm, gn_own, from_lo, from_hi, ga)
    total = lax.optimization_barrier(jnp.sum(shares.astype(F32), axis=0))
    total = lax.optimization_barrier(total.astype(BF16))
    terms = [total.astype(F32)] + [
        lax.ppermute(total, "far", [(i, i ^ k) for i in range(n_far)]).astype(F32)
        for k in range(1, n_far)
    ]
    while len(terms) > 1:
        terms = [terms[i] + terms[i + 1] for i in range(0, len(terms), 2)]
    spread = jnp.broadcast_to(terms[0].astype(BF16), (n_share // 2, *total.shape))
    mine = exchange(spread, ("pair", "chip"))
    theirs = lax.ppermute(mine, "core", [(0, 1), (1, 0)])
    factor = 1.0 / math.sqrt(rows * n_far * lax.axis_size("pair") * n_space)
    outs = pl.pallas_call(
        lambda *refs: unpack_kernel(factor, *refs),
        out_shape=[
            sds((D, 3 * D), F32),
            sds((D, D), F32),
            sds((D, FF), F32),
            sds((FF, D), F32),
            sds((1, D), F32),
            sds((1, D), F32),
        ],
        in_specs=[VM] * 2,
        out_specs=[VM] * 6,
        compiler_params=PARAMS,
        name="unpack",
    )(mine, theirs)
    grad_qkv, grad_out, grad_up, grad_down, grad_ga, grad_gm = outs
    return (output, grad_voxels, grad_qkv, grad_out, grad_up, grad_down, grad_ga.reshape(D), grad_gm.reshape(D))


def solution(mesh):
    n_dp, n_space = mesh.devices.shape
    fine = Mesh(mesh.devices.reshape(n_dp // 2, 2, n_space // 2, 2), ("far", "pair", "chip", "core"))
    row = ("far", "pair", "chip", "core")
    in_specs = (
        P(row, None),
        P(row),
        P(row, None),
        P(),
        P(),
        P(),
        P(),
        P(),
        P(),
        P(row, None),
    )
    out_specs = (P(row, None), P(row, None), P(), P(), P(), P(), P(), P())
    return jax.shard_map(body, mesh=fine, in_specs=in_specs, out_specs=out_specs, check_vma=False)
```

```python
import math

import jax
import jax.numpy as jnp
from jax import lax
from jax.experimental import pallas as pl
from jax.experimental.pallas import tpu as pltpu
from jax.sharding import Mesh, PartitionSpec as P

HEADS = 8
HEAD = 32
BS = 256
PART = 3
SPAN = 2
SLOTS = PART + 1
D = 256
FF = 1024
LANES = 128
EXTRA = 8
PIECE = 32
FAR = 128.0
SHARE = ("core", "pair", "chip")
SPACE = ("chip", "core")

epsilon = 1e-06
root_coef = math.sqrt(2.0 / math.pi)
F32 = jnp.float32
BF16 = jnp.bfloat16
SCORE = 1.0 / math.sqrt(HEAD)
SCORE2 = math.log2(math.e) / math.sqrt(HEAD)


def mm(a, b):
    return lax.dot_general(a, b, (((1,), (0,)), ((), ())), preferred_element_type=F32)


def mm_t(a, b):
    return lax.dot_general(a, b, (((1,), (1,)), ((), ())), preferred_element_type=F32)


def t_mm(a, b):
    return lax.dot_general(a, b, (((0,), (0,)), ((), ())), preferred_element_type=F32)


def put_rows(ref, at, per, vals):
    for i in range(vals.shape[0] // PIECE):
        r = at + i * PIECE
        ref[r // per, r % per : r % per + PIECE, :] = vals[i * PIECE : (i + 1) * PIECE, :]


def main_kernel(local_blocks, partners, counts, xa, lo, hi, gain_attn, w_qkv, w_out, gain_mlp, w_up, w_down, cot,
                output, grads, to_lo, to_hi, gn_own, gm_out,
                bias_s, normed_s, xhat_s, k_s, v_s, kt_s, vt_s, qbt_s, gbt_s, qb_s, gb_s,
                s_s, e_s, ds_s, ot_s, linv_s, del_s, dk_s, dv_s, dqt_s, gnm_s, mix_s, oacc_s):
    nb = local_blocks
    ext = nb + 2 * SPAN
    per = grads.shape[1] - EXTRA
    g_attn = gain_attn[...]
    g_mlp = gain_mlp[...]
    zero_tile = jnp.zeros((D, BS), BF16)
    place = lax.axis_index("far") * lax.axis_size("pair") + lax.axis_index("pair")
    for axis in SPACE:
        place = place * lax.axis_size(axis) + lax.axis_index(axis)
    base = place * nb - SPAN
    lane_head = lax.broadcasted_iota(jnp.int32, (1, D), 1) // HEAD
    row_id = lax.broadcasted_iota(jnp.int32, (BS, BS), 0)

    for blk in range(ext):
        if blk < SPAN:
            src, at = lo, blk
        elif blk < SPAN + nb:
            src, at = xa, blk - SPAN
        else:
            src, at = hi, blk - SPAN - nb
        x = src[at * BS : (at + 1) * BS, :].astype(F32)
        inv = lax.rsqrt(jnp.mean(x * x, axis=-1, keepdims=True) + epsilon)
        xhat = x * inv
        xhat_s[blk] = xhat
        normed = (xhat * g_attn).astype(BF16)
        normed_s[blk] = normed
        if SPAN <= blk < SPAN + nb:
            bias_s[blk] = jnp.where(row_id < counts[at], 0.0, -1e30)
        else:
            bias_s[blk] = jnp.where(x > FAR / 2, -1e30, 0.0)
        k = mm(normed, w_qkv[:, D : 2 * D])
        k_s[blk] = k.astype(BF16)
        kt_s[blk] = k.T.astype(BF16)
        v = mm(normed, w_qkv[:, 2 * D :])
        v_s[blk] = v.astype(BF16)
        vt_s[blk] = v.T.astype(BF16)
        if SPAN <= blk < SPAN + nb:
            q = mm(normed, w_qkv[:, :D])
            qt = q.T.astype(BF16)
            for h in range(HEADS):
                qb_s[at, h] = jnp.where(lane_head == h, q, 0.0).astype(BF16)
                qbt_s[at, h] = zero_tile
                gbt_s[at, h] = zero_tile
                qbt_s[at, h, h * HEAD : (h + 1) * HEAD, :] = qt[h * HEAD : (h + 1) * HEAD, :]
        dk_s[blk] = jnp.zeros((BS, D), F32)
        dv_s[blk] = jnp.zeros((BS, D), F32)

    def slots(b):
        return [b + SPAN] + [partners[b, j] - base for j in range(PART)]

    steps = [(b, h) for b in range(nb) for h in range(HEADS)]
    ids = [slots(b) for b in range(nb)]

    def group(x):
        return x.reshape(BS // 8, 8, BS)

    def score(t):
        b, h = steps[t]
        top = None
        for j in range(SLOTS):
            s = mm(k_s[ids[b][j]], qbt_s[b, h]) + bias_s[ids[b][j]]
            s_s[t % 2, j] = s
            m = jnp.max(group(s), axis=0)
            top = m if top is None else jnp.maximum(top, m)
        return jnp.max(top, axis=0, keepdims=True)

    def weigh(t, top):
        b, h = steps[t]
        total = None
        for j in range(SLOTS):
            e = jnp.exp2((s_s[t % 2, j] - top) * SCORE2)
            e_s[b, h, j] = e.astype(BF16)
            p = jnp.sum(group(e), axis=0)
            total = p if total is None else total + p
        return 1.0 / jnp.sum(total, axis=0, keepdims=True)

    def gather(t, linv):
        b, h = steps[t]
        hs = slice(h * HEAD, (h + 1) * HEAD)
        out = None
        for j in range(SLOTS):
            o = mm(vt_s[ids[b][j], hs, :], e_s[b, h, j])
            out = o if out is None else out + o
        linv_s[t] = linv
        ot_s[b, hs, :] = out * linv

    tops, linvs = {}, {}
    for t in range(len(steps) + 2):
        if t < len(steps):
            tops[t] = score(t)
        if 1 <= t <= len(steps):
            linvs[t - 1] = weigh(t - 1, tops.pop(t - 1))
        if t >= 2:
            gather(t - 2, linvs.pop(t - 2))

    for b in range(nb):
        att = ot_s[b].astype(BF16)
        x = xa[b * BS : (b + 1) * BS, :].astype(F32)
        mixed = x + t_mm(att, w_out[...])
        mix_s[b * BS : (b + 1) * BS, :] = mixed
    mixed = mix_s[...]
    inv_m = lax.rsqrt(jnp.mean(mixed * mixed, axis=-1, keepdims=True) + epsilon)
    nm = (mixed * inv_m * g_mlp).astype(BF16)
    ct = cot[...]
    at_up = 3 * D * D // LANES
    at_down = at_up + D * FF // LANES
    at_out = at_down + D * FF // LANES
    chunk = 256
    for c in range(FF // chunk):
        cs = slice(c * chunk, (c + 1) * chunk)
        pre = mm(nm, w_up[:, cs])
        sq = pre * pre
        tangent = jnp.tanh(root_coef * (pre + 0.044715 * sq * pre))
        half = 0.5 * (1.0 + tangent)
        hidden = (pre * half).astype(BF16)
        slope = half + 0.5 * pre * (1.0 - tangent * tangent) * root_coef * (
            1.0 + 3.0 * 0.044715 * sq
        )
        o = mm(hidden, w_down[cs, :])
        gp = (mm_t(ct, w_down[cs, :]) * slope).astype(BF16)
        g = mm_t(gp, w_up[:, cs])
        if c == 0:
            oacc_s[...] = o
            gnm_s[...] = g
        else:
            oacc_s[...] += o
            gnm_s[...] += g
        down = t_mm(hidden, ct).astype(BF16)
        up = t_mm(nm, gp).astype(BF16)
        for i in range(D // LANES):
            put_rows(grads, at_down + i * FF + c * chunk, per, down[:, i * LANES : (i + 1) * LANES])
        for i in range(chunk // LANES):
            put_rows(grads, at_up + (c * (chunk // LANES) + i) * D, per, up[:, i * LANES : (i + 1) * LANES])
    output[...] = (mixed + oacc_s[...]).astype(BF16)
    gnm = gnm_s[...]
    scaled = gnm * g_mlp
    gm = ct.astype(F32) + inv_m * (
        scaled - mixed * (inv_m * inv_m) * jnp.mean(scaled * mixed, axis=-1, keepdims=True)
    )
    gm_out[...] = gm
    gain_mlp_sum = jnp.sum(gnm * mixed * inv_m, axis=0, keepdims=True)
    gmb = gm.astype(BF16)
    out_sum = None
    for b in range(nb):
        g_b = gmb[b * BS : (b + 1) * BS, :]
        o = mm(ot_s[b].astype(BF16), g_b)
        out_sum = o if out_sum is None else out_sum + o
        gt = mm_t(w_out[...], g_b).astype(BF16).astype(F32)
        pieces = []
        for h in range(HEADS):
            hs = slice(h * HEAD, (h + 1) * HEAD)
            gh = (gt[hs, :] * linv_s[b * HEADS + h]).astype(BF16)
            gbt_s[b, h, hs, :] = gh
            gf = gh.astype(F32)
            pieces.append(gf)
            del_s[b * HEADS + h] = jnp.sum(gf * ot_s[b, hs, :], axis=0, keepdims=True)
        gq = jnp.concatenate(pieces, axis=0).T
        for h in range(HEADS):
            gb_s[b, h] = jnp.where(lane_head == h, gq, 0.0).astype(BF16)
    out_sum = out_sum.astype(BF16)
    for i in range(D // LANES):
        put_rows(grads, at_out + i * D, per, out_sum[:, i * LANES : (i + 1) * LANES])

    def score_grad(t):
        b, h = steps[t]
        for j in range(SLOTS):
            gw = mm(v_s[ids[b][j]], gbt_s[b, h])
            ds_s[b, h, j] = (e_s[b, h, j].astype(F32) * (gw - del_s[t])).astype(BF16)

    def query_grad(t):
        b, h = steps[t]
        hs = slice(h * HEAD, (h + 1) * HEAD)
        dq = None
        for j in range(SLOTS):
            q = mm(kt_s[ids[b][j], hs, :], ds_s[b, h, j])
            dq = q if dq is None else dq + q
        dqt_s[b, hs, :] = dq * SCORE

    for t in range(len(steps) + 1):
        if t < len(steps):
            score_grad(t)
        if t >= 1:
            query_grad(t - 1)

    for b in range(nb):
        for j in range(SLOTS):
            dv = None
            dk = None
            for h in range(HEADS):
                a = mm(e_s[b, h, j], gb_s[b, h])
                dv = a if dv is None else dv + a
            for h in range(HEADS):
                a = mm(ds_s[b, h, j], qb_s[b, h])
                dk = a if dk is None else dk + a
            dv_s[ids[b][j]] += dv
            dk_s[ids[b][j]] += dk

    wq = w_qkv[:, :D]
    wk = w_qkv[:, D : 2 * D]
    wv = w_qkv[:, 2 * D :]
    sums = [None, None, None]
    gain_sum = None
    for blk in range(ext):
        normed = normed_s[blk]
        dk = (dk_s[blk] * SCORE).astype(BF16)
        dv = dv_s[blk].astype(BF16)
        gn = mm_t(dk, wk) + mm_t(dv, wv)
        parts = [(1, dk), (2, dv)]
        if SPAN <= blk < SPAN + nb:
            dq = dqt_s[blk - SPAN].T.astype(BF16)
            gn = gn + mm_t(dq, wq)
            parts.append((0, dq))
            gn_own[(blk - SPAN) * BS : (blk - SPAN + 1) * BS, :] = gn
        elif blk < SPAN:
            to_lo[blk * BS : (blk + 1) * BS, :] = gn.astype(BF16)
        else:
            to_hi[(blk - SPAN - nb) * BS : (blk - SPAN - nb + 1) * BS, :] = gn.astype(BF16)
        for which, val in parts:
            a = t_mm(normed, val)
            sums[which] = a if sums[which] is None else sums[which] + a
        g = jnp.sum(gn * xhat_s[blk], axis=0, keepdims=True)
        gain_sum = g if gain_sum is None else gain_sum + g
    for which in range(3):
        s = sums[which].astype(BF16)
        for i in range(D // LANES):
            put_rows(grads, (which * (D // LANES) + i) * D, per, s[:, i * LANES : (i + 1) * LANES])
    for r in range(grads.shape[0]):
        grads[r, per:, :] = jnp.zeros((EXTRA, LANES), BF16)
    for i in range(D // LANES):
        ls = slice(i * LANES, (i + 1) * LANES)
        grads[i, per:, :] = jnp.broadcast_to(gain_sum[:, ls], (EXTRA, LANES)).astype(BF16)
        grads[D // LANES + i, per:, :] = jnp.broadcast_to(gain_mlp_sum[:, ls], (EXTRA, LANES)).astype(BF16)


def back_kernel(xa, gm, scaled_own, from_lo, from_hi, gain_attn, grad_voxels):
    x = xa[...].astype(F32)
    inv = lax.rsqrt(jnp.mean(x * x, axis=-1, keepdims=True) + epsilon)
    halo = from_lo[...].astype(F32) + from_hi[...].astype(F32)
    scaled = scaled_own[...] + halo * gain_attn[...]
    grad_voxels[...] = gm[...] + inv * (
        scaled - x * (inv * inv) * jnp.mean(scaled * x, axis=-1, keepdims=True)
    )


def get_rows(halves, at, per, count):
    half = halves[0].shape[0]
    out = []
    for i in range(count // PIECE):
        r = at + i * PIECE
        share = r // per
        ref = halves[share // half]
        out.append(ref[share % half, r % per : r % per + PIECE, :].astype(F32))
    return jnp.concatenate(out, axis=0)


def unpack_kernel(factor, mine, theirs, grad_qkv, grad_out, grad_up, grad_down, grad_ga, grad_gm):
    per = mine.shape[1] - EXTRA
    at_up = 3 * D * D // LANES
    at_down = at_up + D * FF // LANES
    at_out = at_down + D * FF // LANES

    def unpack(halves):
        for i in range(3 * D // LANES):
            grad_qkv[:, i * LANES : (i + 1) * LANES] = get_rows(halves, i * D, per, D) * factor
        for i in range(FF // LANES):
            grad_up[:, i * LANES : (i + 1) * LANES] = get_rows(halves, at_up + i * D, per, D) * factor
        for i in range(D // LANES):
            ls = slice(i * LANES, (i + 1) * LANES)
            grad_down[:, ls] = get_rows(halves, at_down + i * FF, per, FF) * factor
            grad_out[:, ls] = get_rows(halves, at_out + i * D, per, D) * factor
            grad_ga[:, ls] = halves[0][i, per : per + 1, :].astype(F32) * factor
            grad_gm[:, ls] = halves[0][D // LANES + i, per : per + 1, :].astype(F32) * factor

    core = lax.axis_index("core")
    pl.when(core == 0)(lambda: unpack((mine, theirs)))
    pl.when(core != 0)(lambda: unpack((theirs, mine)))


VM = pl.BlockSpec(memory_space=pltpu.VMEM)
SM = pl.BlockSpec(memory_space=pltpu.SMEM)
PARAMS = pltpu.CompilerParams(vmem_limit_bytes=60 * 1024 * 1024)


def sds(shape, dtype):
    return jax.ShapeDtypeStruct(shape, dtype)


def exchange(x, axis):
    return lax.all_to_all(x, axis, split_axis=0, concat_axis=0, tiled=True)


def body(voxels, counts, partners, gain_attn, w_qkv, w_out, gain_mlp, w_up, w_down, cotangent):
    nb = counts.shape[0]
    rows = voxels.shape[0]
    n_space = lax.axis_size(SPACE)
    n_share = lax.axis_size(SHARE)
    n_far = lax.axis_size("far")
    up = [(i, i + 1) for i in range(n_space - 1)]
    down = [(j, i) for i, j in up]
    held = lax.broadcasted_iota(jnp.int32, (nb, BS, D), 1) < counts[:, None, None]
    marked = jnp.where(held, voxels.reshape(nb, BS, D), jnp.asarray(FAR, BF16)).reshape(rows, D)
    lo = lax.ppermute(marked, SPACE, up)
    hi = lax.ppermute(marked, SPACE, down)
    ext = nb + 2 * SPAN
    per = (3 * D * D + D * D + 2 * D * FF) // LANES // n_share
    tile = (BS, D)
    scratch = [
        pltpu.VMEM((ext, *tile), F32),
        pltpu.VMEM((ext, *tile), BF16),
        pltpu.VMEM((ext, *tile), F32),
        pltpu.VMEM((ext, *tile), BF16),
        pltpu.VMEM((ext, *tile), BF16),
        pltpu.VMEM((ext, *tile), BF16),
        pltpu.VMEM((ext, *tile), BF16),
        pltpu.VMEM((nb, HEADS, *tile), BF16),
        pltpu.VMEM((nb, HEADS, *tile), BF16),
        pltpu.VMEM((nb, HEADS, *tile), BF16),
        pltpu.VMEM((nb, HEADS, *tile), BF16),
        pltpu.VMEM((2, SLOTS, BS, BS), F32),
        pltpu.VMEM((nb, HEADS, SLOTS, BS, BS), BF16),
        pltpu.VMEM((nb, HEADS, SLOTS, BS, BS), BF16),
        pltpu.VMEM((nb, *tile), F32),
        pltpu.VMEM((nb * HEADS, 1, BS), F32),
        pltpu.VMEM((nb * HEADS, 1, BS), F32),
        pltpu.VMEM((ext, *tile), F32),
        pltpu.VMEM((ext, *tile), F32),
        pltpu.VMEM((nb, *tile), F32),
        pltpu.VMEM((rows, D), F32),
        pltpu.VMEM((rows, D), F32),
        pltpu.VMEM((rows, D), F32),
    ]
    ga = gain_attn.reshape(1, D)
    gmlp = gain_mlp.reshape(1, D)
    output, grads, to_lo, to_hi, gn_own, gm = pl.pallas_call(
        lambda *refs: main_kernel(nb, *refs),
        out_shape=[
            sds((rows, D), BF16),
            sds((n_share, per + EXTRA, LANES), BF16),
            sds((rows, D), BF16),
            sds((rows, D), BF16),
            sds((rows, D), F32),
            sds((rows, D), F32),
        ],
        in_specs=[SM, SM] + [VM] * 10,
        out_specs=[VM] * 6,
        scratch_shapes=scratch,
        compiler_params=PARAMS,
        name="layer",
    )(partners, counts, voxels, lo, hi, ga, w_qkv, w_out, gmlp, w_up, w_down, cotangent)
    core = lax.axis_index("core")
    halves = grads.reshape(2, n_share // 2, *grads.shape[1:])
    got = lax.ppermute(lax.dynamic_index_in_dim(halves, 1 - core, 0, False), "core", [(0, 1), (1, 0)])
    kept = lax.dynamic_index_in_dim(halves, core, 0, False)
    half = (kept.astype(F32) + got.astype(F32)).astype(BF16)
    shares = exchange(half, ("pair", "chip"))
    from_lo = lax.ppermute(to_hi, SPACE, up)
    from_hi = lax.ppermute(to_lo, SPACE, down)
    scaled_own = lax.optimization_barrier(gn_own * ga)
    total = lax.optimization_barrier(jnp.sum(shares.astype(F32), axis=0))
    total = lax.optimization_barrier(total.astype(BF16))
    terms = [total.astype(F32)] + [
        lax.ppermute(total, "far", [(i, i ^ k) for i in range(n_far)]).astype(F32)
        for k in range(1, n_far)
    ]
    while len(terms) > 1:
        terms = [terms[i] + terms[i + 1] for i in range(0, len(terms), 2)]
    spread = jnp.broadcast_to(terms[0].astype(BF16), (n_share // 2, *total.shape))
    mine = exchange(spread, ("pair", "chip"))
    theirs = lax.ppermute(mine, "core", [(0, 1), (1, 0)])
    grad_voxels = pl.pallas_call(
        back_kernel,
        out_shape=sds((rows, D), F32),
        in_specs=[VM] * 6,
        out_specs=VM,
        compiler_params=PARAMS,
        cost_estimate=pl.CostEstimate(flops=4000000, transcendentals=0, bytes_accessed=3000000),
        name="voxel_grad",
    )(voxels, gm, scaled_own, from_lo, from_hi, ga)
    factor = 1.0 / math.sqrt(rows * n_far * lax.axis_size("pair") * n_space)
    outs = pl.pallas_call(
        lambda *refs: unpack_kernel(factor, *refs),
        out_shape=[
            sds((D, 3 * D), F32),
            sds((D, D), F32),
            sds((D, FF), F32),
            sds((FF, D), F32),
            sds((1, D), F32),
            sds((1, D), F32),
        ],
        in_specs=[VM] * 2,
        out_specs=[VM] * 6,
        compiler_params=PARAMS,
        name="unpack",
    )(mine, theirs)
    grad_qkv, grad_out, grad_up, grad_down, grad_ga, grad_gm = outs
    return (output, grad_voxels, grad_qkv, grad_out, grad_up, grad_down, grad_ga.reshape(D), grad_gm.reshape(D))


def solution(mesh):
    n_dp, n_space = mesh.devices.shape
    fine = Mesh(mesh.devices.reshape(n_dp // 2, 2, n_space // 2, 2), ("far", "pair", "chip", "core"))
    row = ("far", "pair", "chip", "core")
    in_specs = (
        P(row, None),
        P(row),
        P(row, None),
        P(),
        P(),
        P(),
        P(),
        P(),
        P(),
        P(row, None),
    )
    out_specs = (P(row, None), P(row, None), P(), P(), P(), P(), P(), P())
    return jax.shard_map(body, mesh=fine, in_specs=in_specs, out_specs=out_specs, check_vma=False)
```

```python
import math

import jax
import jax.numpy as jnp
from jax import lax
from jax.experimental import pallas as pl
from jax.experimental.pallas import tpu as pltpu
from jax.sharding import Mesh, PartitionSpec as P

HEADS = 8
HEAD = 32
BS = 256
PART = 3
SPAN = 2
SLOTS = PART + 1
D = 256
FF = 1024
LANES = 128
EXTRA = 8
PIECE = 32
FAR = 128.0
SHARE = ("core", "pair", "chip")
SPACE = ("chip", "core")

epsilon = 1e-06
root_coef = math.sqrt(2.0 / math.pi)
F32 = jnp.float32
BF16 = jnp.bfloat16
SCORE = 1.0 / math.sqrt(HEAD)
SCORE2 = math.log2(math.e) / math.sqrt(HEAD)


def mm(a, b):
    return lax.dot_general(a, b, (((1,), (0,)), ((), ())), preferred_element_type=F32)


def mm_t(a, b):
    return lax.dot_general(a, b, (((1,), (1,)), ((), ())), preferred_element_type=F32)


def t_mm(a, b):
    return lax.dot_general(a, b, (((0,), (0,)), ((), ())), preferred_element_type=F32)


def put_rows(ref, at, per, vals):
    for i in range(vals.shape[0] // PIECE):
        r = at + i * PIECE
        ref[r // per, r % per : r % per + PIECE, :] = vals[i * PIECE : (i + 1) * PIECE, :]


def main_kernel(local_blocks, partners, counts, xa, lo, hi, gain_attn, w_qkv, gain_mlp,
                w_out_any, w_up_any, w_down_any, cot_any,
                grads, to_lo, to_hi, gn_own, output_any, gm_any,
                w_out, w_up, w_down, cot, output, gm_out, in_sems, out_sems,
                bias_s, normed_s, xhat_s, k_s, v_s, kt_s, vt_s, qbt_s, gbt_s, qb_s, gb_s,
                s_s, e_s, ds_s, ot_s, linv_s, del_s, dk_s, dv_s, dqt_s, gnm_s, mix_s, oacc_s):
    nb = local_blocks
    ext = nb + 2 * SPAN
    late = [(w_out_any, w_out), (w_up_any, w_up), (w_down_any, w_down), (cot_any, cot)]
    late = [pltpu.make_async_copy(*pair, in_sems.at[i]) for i, pair in enumerate(late)]
    for copy in late:
        copy.start()
    early = [(output, output_any), (gm_out, gm_any)]
    early = [pltpu.make_async_copy(*pair, out_sems.at[i]) for i, pair in enumerate(early)]
    per = grads.shape[1] - EXTRA
    g_attn = gain_attn[...]
    g_mlp = gain_mlp[...]
    zero_tile = jnp.zeros((D, BS), BF16)
    place = lax.axis_index("far") * lax.axis_size("pair") + lax.axis_index("pair")
    for axis in SPACE:
        place = place * lax.axis_size(axis) + lax.axis_index(axis)
    base = place * nb - SPAN
    lane_head = lax.broadcasted_iota(jnp.int32, (1, D), 1) // HEAD
    row_id = lax.broadcasted_iota(jnp.int32, (BS, BS), 0)

    for blk in range(ext):
        if blk < SPAN:
            src, at = lo, blk
        elif blk < SPAN + nb:
            src, at = xa, blk - SPAN
        else:
            src, at = hi, blk - SPAN - nb
        x = src[at * BS : (at + 1) * BS, :].astype(F32)
        inv = lax.rsqrt(jnp.mean(x * x, axis=-1, keepdims=True) + epsilon)
        xhat = x * inv
        xhat_s[blk] = xhat
        normed = (xhat * g_attn).astype(BF16)
        normed_s[blk] = normed
        if SPAN <= blk < SPAN + nb:
            bias_s[blk] = jnp.where(row_id < counts[at], 0.0, -1e30)
        else:
            bias_s[blk] = jnp.where(x > FAR / 2, -1e30, 0.0)
        k = mm(normed, w_qkv[:, D : 2 * D])
        k_s[blk] = k.astype(BF16)
        kt_s[blk] = k.T.astype(BF16)
        v = mm(normed, w_qkv[:, 2 * D :])
        v_s[blk] = v.astype(BF16)
        vt_s[blk] = v.T.astype(BF16)
        if SPAN <= blk < SPAN + nb:
            q = mm(normed, w_qkv[:, :D])
            qt = q.T.astype(BF16)
            for h in range(HEADS):
                qb_s[at, h] = jnp.where(lane_head == h, q, 0.0).astype(BF16)
                qbt_s[at, h] = zero_tile
                gbt_s[at, h] = zero_tile
                qbt_s[at, h, h * HEAD : (h + 1) * HEAD, :] = qt[h * HEAD : (h + 1) * HEAD, :]
        dk_s[blk] = jnp.zeros((BS, D), F32)
        dv_s[blk] = jnp.zeros((BS, D), F32)

    def slots(b):
        return [b + SPAN] + [partners[b, j] - base for j in range(PART)]

    steps = [(b, h) for b in range(nb) for h in range(HEADS)]
    ids = [slots(b) for b in range(nb)]

    def group(x):
        return x.reshape(BS // 8, 8, BS)

    def score(t):
        b, h = steps[t]
        top = None
        for j in range(SLOTS):
            s = mm(k_s[ids[b][j]], qbt_s[b, h]) + bias_s[ids[b][j]]
            s_s[t % 2, j] = s
            m = jnp.max(group(s), axis=0)
            top = m if top is None else jnp.maximum(top, m)
        return jnp.max(top, axis=0, keepdims=True)

    def weigh(t, top):
        b, h = steps[t]
        total = None
        for j in range(SLOTS):
            e = jnp.exp2((s_s[t % 2, j] - top) * SCORE2)
            e_s[b, h, j] = e.astype(BF16)
            p = jnp.sum(group(e), axis=0)
            total = p if total is None else total + p
        return 1.0 / jnp.sum(total, axis=0, keepdims=True)

    def gather(t, linv):
        b, h = steps[t]
        hs = slice(h * HEAD, (h + 1) * HEAD)
        out = None
        for j in range(SLOTS):
            o = mm(vt_s[ids[b][j], hs, :], e_s[b, h, j])
            out = o if out is None else out + o
        linv_s[t] = linv
        ot_s[b, hs, :] = out * linv

    tops, linvs = {}, {}
    for t in range(len(steps) + 2):
        if t < len(steps):
            tops[t] = score(t)
        if 1 <= t <= len(steps):
            linvs[t - 1] = weigh(t - 1, tops.pop(t - 1))
        if t >= 2:
            gather(t - 2, linvs.pop(t - 2))

    for copy in late:
        copy.wait()
    for b in range(nb):
        att = ot_s[b].astype(BF16)
        x = xa[b * BS : (b + 1) * BS, :].astype(F32)
        mixed = x + t_mm(att, w_out[...])
        mix_s[b * BS : (b + 1) * BS, :] = mixed
    mixed = mix_s[...]
    inv_m = lax.rsqrt(jnp.mean(mixed * mixed, axis=-1, keepdims=True) + epsilon)
    nm = (mixed * inv_m * g_mlp).astype(BF16)
    ct = cot[...]
    at_up = 3 * D * D // LANES
    at_down = at_up + D * FF // LANES
    at_out = at_down + D * FF // LANES
    chunk = 256
    for c in range(FF // chunk):
        cs = slice(c * chunk, (c + 1) * chunk)
        pre = mm(nm, w_up[:, cs])
        sq = pre * pre
        tangent = jnp.tanh(root_coef * (pre + 0.044715 * sq * pre))
        half = 0.5 * (1.0 + tangent)
        hidden = (pre * half).astype(BF16)
        slope = half + 0.5 * pre * (1.0 - tangent * tangent) * root_coef * (
            1.0 + 3.0 * 0.044715 * sq
        )
        o = mm(hidden, w_down[cs, :])
        gp = (mm_t(ct, w_down[cs, :]) * slope).astype(BF16)
        g = mm_t(gp, w_up[:, cs])
        if c == 0:
            oacc_s[...] = o
            gnm_s[...] = g
        else:
            oacc_s[...] += o
            gnm_s[...] += g
        down = t_mm(hidden, ct).astype(BF16)
        up = t_mm(nm, gp).astype(BF16)
        for i in range(D // LANES):
            put_rows(grads, at_down + i * FF + c * chunk, per, down[:, i * LANES : (i + 1) * LANES])
        for i in range(chunk // LANES):
            put_rows(grads, at_up + (c * (chunk // LANES) + i) * D, per, up[:, i * LANES : (i + 1) * LANES])
    output[...] = (mixed + oacc_s[...]).astype(BF16)
    early[0].start()
    gnm = gnm_s[...]
    scaled = gnm * g_mlp
    gm = ct.astype(F32) + inv_m * (
        scaled - mixed * (inv_m * inv_m) * jnp.mean(scaled * mixed, axis=-1, keepdims=True)
    )
    gm_out[...] = gm
    early[1].start()
    gain_mlp_sum = jnp.sum(gnm * mixed * inv_m, axis=0, keepdims=True)
    gmb = gm.astype(BF16)
    out_sum = None
    for b in range(nb):
        g_b = gmb[b * BS : (b + 1) * BS, :]
        o = mm(ot_s[b].astype(BF16), g_b)
        out_sum = o if out_sum is None else out_sum + o
        gt = mm_t(w_out[...], g_b).astype(BF16).astype(F32)
        pieces = []
        for h in range(HEADS):
            hs = slice(h * HEAD, (h + 1) * HEAD)
            gh = (gt[hs, :] * linv_s[b * HEADS + h]).astype(BF16)
            gbt_s[b, h, hs, :] = gh
            gf = gh.astype(F32)
            pieces.append(gf)
            del_s[b * HEADS + h] = jnp.sum(gf * ot_s[b, hs, :], axis=0, keepdims=True)
        gq = jnp.concatenate(pieces, axis=0).T
        for h in range(HEADS):
            gb_s[b, h] = jnp.where(lane_head == h, gq, 0.0).astype(BF16)
    out_sum = out_sum.astype(BF16)
    for i in range(D // LANES):
        put_rows(grads, at_out + i * D, per, out_sum[:, i * LANES : (i + 1) * LANES])

    def score_grad(t):
        b, h = steps[t]
        for j in range(SLOTS):
            gw = mm(v_s[ids[b][j]], gbt_s[b, h])
            ds_s[b, h, j] = (e_s[b, h, j].astype(F32) * (gw - del_s[t])).astype(BF16)

    def query_grad(t):
        b, h = steps[t]
        hs = slice(h * HEAD, (h + 1) * HEAD)
        dq = None
        for j in range(SLOTS):
            q = mm(kt_s[ids[b][j], hs, :], ds_s[b, h, j])
            dq = q if dq is None else dq + q
        dqt_s[b, hs, :] = dq * SCORE

    for t in range(len(steps) + 1):
        if t < len(steps):
            score_grad(t)
        if t >= 1:
            query_grad(t - 1)

    for b in range(nb):
        for j in range(SLOTS):
            dv = None
            dk = None
            for h in range(HEADS):
                a = mm(e_s[b, h, j], gb_s[b, h])
                dv = a if dv is None else dv + a
            for h in range(HEADS):
                a = mm(ds_s[b, h, j], qb_s[b, h])
                dk = a if dk is None else dk + a
            dv_s[ids[b][j]] += dv
            dk_s[ids[b][j]] += dk

    wq = w_qkv[:, :D]
    wk = w_qkv[:, D : 2 * D]
    wv = w_qkv[:, 2 * D :]
    sums = [None, None, None]
    gain_sum = None
    for blk in range(ext):
        normed = normed_s[blk]
        dk = (dk_s[blk] * SCORE).astype(BF16)
        dv = dv_s[blk].astype(BF16)
        gn = mm_t(dk, wk) + mm_t(dv, wv)
        parts = [(1, dk), (2, dv)]
        if SPAN <= blk < SPAN + nb:
            dq = dqt_s[blk - SPAN].T.astype(BF16)
            gn = gn + mm_t(dq, wq)
            parts.append((0, dq))
            gn_own[(blk - SPAN) * BS : (blk - SPAN + 1) * BS, :] = gn
        elif blk < SPAN:
            to_lo[blk * BS : (blk + 1) * BS, :] = gn.astype(BF16)
        else:
            to_hi[(blk - SPAN - nb) * BS : (blk - SPAN - nb + 1) * BS, :] = gn.astype(BF16)
        for which, val in parts:
            a = t_mm(normed, val)
            sums[which] = a if sums[which] is None else sums[which] + a
        g = jnp.sum(gn * xhat_s[blk], axis=0, keepdims=True)
        gain_sum = g if gain_sum is None else gain_sum + g
    for which in range(3):
        s = sums[which].astype(BF16)
        for i in range(D // LANES):
            put_rows(grads, (which * (D // LANES) + i) * D, per, s[:, i * LANES : (i + 1) * LANES])
    for r in range(grads.shape[0]):
        grads[r, per:, :] = jnp.zeros((EXTRA, LANES), BF16)
    for i in range(D // LANES):
        ls = slice(i * LANES, (i + 1) * LANES)
        grads[i, per:, :] = jnp.broadcast_to(gain_sum[:, ls], (EXTRA, LANES)).astype(BF16)
        grads[D // LANES + i, per:, :] = jnp.broadcast_to(gain_mlp_sum[:, ls], (EXTRA, LANES)).astype(BF16)
    for copy in early:
        copy.wait()


def back_kernel(xa, gm, scaled_own, from_lo, from_hi, gain_attn, grad_voxels):
    x = xa[...].astype(F32)
    inv = lax.rsqrt(jnp.mean(x * x, axis=-1, keepdims=True) + epsilon)
    halo = from_lo[...].astype(F32) + from_hi[...].astype(F32)
    scaled = scaled_own[...] + halo * gain_attn[...]
    grad_voxels[...] = gm[...] + inv * (
        scaled - x * (inv * inv) * jnp.mean(scaled * x, axis=-1, keepdims=True)
    )


def get_rows(halves, at, per, count):
    half = halves[0].shape[0]
    out = []
    for i in range(count // PIECE):
        r = at + i * PIECE
        share = r // per
        ref = halves[share // half]
        out.append(ref[share % half, r % per : r % per + PIECE, :].astype(F32))
    return jnp.concatenate(out, axis=0)


def unpack_kernel(factor, mine, theirs, *refs):
    outs, bufs, sems = refs[:6], refs[6:12], refs[12]
    grad_qkv, grad_out, grad_up, grad_down, grad_ga, grad_gm = bufs
    per = mine.shape[1] - EXTRA
    at_up = 3 * D * D // LANES
    at_down = at_up + D * FF // LANES
    at_out = at_down + D * FF // LANES
    copies = [pltpu.make_async_copy(b, o, sems.at[i]) for i, (b, o) in enumerate(zip(bufs, outs))]

    def unpack(halves):
        for i in range(FF // LANES):
            grad_up[:, i * LANES : (i + 1) * LANES] = get_rows(halves, at_up + i * D, per, D) * factor
        copies[2].start()
        for i in range(D // LANES):
            grad_down[:, i * LANES : (i + 1) * LANES] = get_rows(halves, at_down + i * FF, per, FF) * factor
        copies[3].start()
        for i in range(3 * D // LANES):
            grad_qkv[:, i * LANES : (i + 1) * LANES] = get_rows(halves, i * D, per, D) * factor
        copies[0].start()
        for i in range(D // LANES):
            ls = slice(i * LANES, (i + 1) * LANES)
            grad_out[:, ls] = get_rows(halves, at_out + i * D, per, D) * factor
            grad_ga[:, ls] = halves[0][i, per : per + 1, :].astype(F32) * factor
            grad_gm[:, ls] = halves[0][D // LANES + i, per : per + 1, :].astype(F32) * factor
        for i in (1, 4, 5):
            copies[i].start()

    core = lax.axis_index("core")
    pl.when(core == 0)(lambda: unpack((mine, theirs)))
    pl.when(core != 0)(lambda: unpack((theirs, mine)))
    for copy in copies:
        copy.wait()


VM = pl.BlockSpec(memory_space=pltpu.VMEM)
SM = pl.BlockSpec(memory_space=pltpu.SMEM)
ANY = pl.BlockSpec(memory_space=pl.ANY)
PARAMS = pltpu.CompilerParams(vmem_limit_bytes=60 * 1024 * 1024)


def sds(shape, dtype):
    return jax.ShapeDtypeStruct(shape, dtype)


def exchange(x, axis):
    return lax.all_to_all(x, axis, split_axis=0, concat_axis=0, tiled=True)


def body(voxels, counts, partners, gain_attn, w_qkv, w_out, gain_mlp, w_up, w_down, cotangent):
    nb = counts.shape[0]
    rows = voxels.shape[0]
    n_space = lax.axis_size(SPACE)
    n_share = lax.axis_size(SHARE)
    n_far = lax.axis_size("far")
    up = [(i, i + 1) for i in range(n_space - 1)]
    down = [(j, i) for i, j in up]
    held = lax.broadcasted_iota(jnp.int32, (nb, BS, D), 1) < counts[:, None, None]
    marked = jnp.where(held, voxels.reshape(nb, BS, D), jnp.asarray(FAR, BF16)).reshape(rows, D)
    lo = lax.ppermute(marked, SPACE, up)
    hi = lax.ppermute(marked, SPACE, down)
    ext = nb + 2 * SPAN
    per = (3 * D * D + D * D + 2 * D * FF) // LANES // n_share
    tile = (BS, D)
    scratch = [
        pltpu.VMEM((ext, *tile), F32),
        pltpu.VMEM((ext, *tile), BF16),
        pltpu.VMEM((ext, *tile), F32),
        pltpu.VMEM((ext, *tile), BF16),
        pltpu.VMEM((ext, *tile), BF16),
        pltpu.VMEM((ext, *tile), BF16),
        pltpu.VMEM((ext, *tile), BF16),
        pltpu.VMEM((nb, HEADS, *tile), BF16),
        pltpu.VMEM((nb, HEADS, *tile), BF16),
        pltpu.VMEM((nb, HEADS, *tile), BF16),
        pltpu.VMEM((nb, HEADS, *tile), BF16),
        pltpu.VMEM((2, SLOTS, BS, BS), F32),
        pltpu.VMEM((nb, HEADS, SLOTS, BS, BS), BF16),
        pltpu.VMEM((nb, HEADS, SLOTS, BS, BS), BF16),
        pltpu.VMEM((nb, *tile), F32),
        pltpu.VMEM((nb * HEADS, 1, BS), F32),
        pltpu.VMEM((nb * HEADS, 1, BS), F32),
        pltpu.VMEM((ext, *tile), F32),
        pltpu.VMEM((ext, *tile), F32),
        pltpu.VMEM((nb, *tile), F32),
        pltpu.VMEM((rows, D), F32),
        pltpu.VMEM((rows, D), F32),
        pltpu.VMEM((rows, D), F32),
    ]
    ga = gain_attn.reshape(1, D)
    gmlp = gain_mlp.reshape(1, D)
    own_copies = [
        pltpu.VMEM(w_out.shape, BF16),
        pltpu.VMEM(w_up.shape, BF16),
        pltpu.VMEM(w_down.shape, BF16),
        pltpu.VMEM((rows, D), BF16),
        pltpu.VMEM((rows, D), BF16),
        pltpu.VMEM((rows, D), F32),
        pltpu.SemaphoreType.DMA((4,)),
        pltpu.SemaphoreType.DMA((2,)),
    ]
    grads, to_lo, to_hi, gn_own, output, gm = pl.pallas_call(
        lambda *refs: main_kernel(nb, *refs),
        out_shape=[
            sds((n_share, per + EXTRA, LANES), BF16),
            sds((rows, D), BF16),
            sds((rows, D), BF16),
            sds((rows, D), F32),
            sds((rows, D), BF16),
            sds((rows, D), F32),
        ],
        in_specs=[SM, SM] + [VM] * 6 + [ANY] * 4,
        out_specs=[VM] * 4 + [ANY] * 2,
        scratch_shapes=own_copies + scratch,
        compiler_params=PARAMS,
        name="layer",
    )(partners, counts, voxels, lo, hi, ga, w_qkv, gmlp, w_out, w_up, w_down, cotangent)
    core = lax.axis_index("core")
    halves = grads.reshape(2, n_share // 2, *grads.shape[1:])
    got = lax.ppermute(lax.dynamic_index_in_dim(halves, 1 - core, 0, False), "core", [(0, 1), (1, 0)])
    kept = lax.dynamic_index_in_dim(halves, core, 0, False)
    half = (kept.astype(F32) + got.astype(F32)).astype(BF16)
    shares = exchange(half, ("pair", "chip"))
    from_lo = lax.ppermute(to_hi, SPACE, up)
    from_hi = lax.ppermute(to_lo, SPACE, down)
    scaled_own = lax.optimization_barrier(gn_own * ga)
    total = lax.optimization_barrier(jnp.sum(shares.astype(F32), axis=0))
    total = lax.optimization_barrier(total.astype(BF16))
    terms = [total] + [
        lax.ppermute(total, "far", [(i, i ^ k) for i in range(n_far)]) for k in range(1, n_far)
    ]
    terms = [term.astype(F32) for term in terms]
    while len(terms) > 1:
        terms = [terms[i] + terms[i + 1] for i in range(0, len(terms), 2)]
    spread = jnp.broadcast_to(terms[0].astype(BF16), (n_share // 2, *total.shape))
    mine = exchange(spread, ("pair", "chip"))
    theirs = lax.ppermute(mine, "core", [(0, 1), (1, 0)])
    grad_voxels = pl.pallas_call(
        back_kernel,
        out_shape=sds((rows, D), F32),
        in_specs=[VM] * 6,
        out_specs=VM,
        compiler_params=PARAMS,
        cost_estimate=pl.CostEstimate(flops=4000000, transcendentals=0, bytes_accessed=3000000),
        name="voxel_grad",
    )(voxels, gm, scaled_own, from_lo, from_hi, ga)
    factor = 1.0 / math.sqrt(rows * n_far * lax.axis_size("pair") * n_space)
    shapes = [(D, 3 * D), (D, D), (D, FF), (FF, D), (1, D), (1, D)]
    outs = pl.pallas_call(
        lambda *refs: unpack_kernel(factor, *refs),
        out_shape=[sds(shape, F32) for shape in shapes],
        in_specs=[VM] * 2,
        out_specs=[ANY] * 6,
        scratch_shapes=[pltpu.VMEM(shape, F32) for shape in shapes] + [pltpu.SemaphoreType.DMA((6,))],
        compiler_params=PARAMS,
        name="unpack",
    )(mine, theirs)
    grad_qkv, grad_out, grad_up, grad_down, grad_ga, grad_gm = outs
    return (output, grad_voxels, grad_qkv, grad_out, grad_up, grad_down, grad_ga.reshape(D), grad_gm.reshape(D))


def solution(mesh):
    n_dp, n_space = mesh.devices.shape
    fine = Mesh(mesh.devices.reshape(n_dp // 2, 2, n_space // 2, 2), ("far", "pair", "chip", "core"))
    row = ("far", "pair", "chip", "core")
    in_specs = (
        P(row, None),
        P(row),
        P(row, None),
        P(),
        P(),
        P(),
        P(),
        P(),
        P(),
        P(row, None),
    )
    out_specs = (P(row, None), P(row, None), P(), P(), P(), P(), P(), P())
    return jax.shard_map(body, mesh=fine, in_specs=in_specs, out_specs=out_specs, check_vma=False)
```
